8 devices in a mesh: mp: 1 (over z), dpa: 2 (over y), dpb: 2 (over x), dpc: 2 (over core).
Axes of the slice: x: 2, y: 2, z: 1, core: 2. Of those that a mesh axis runs over, the one named last changes fastest.
Arguments:
- x: bfloat16 [65536, 768], P(('mp', 'dpa', 'dpb', 'dpc'))
- g: bfloat16 [65536, 768], P(('mp', 'dpa', 'dpb', 'dpc'))
- w1: bfloat16 [768, 3072], P('mp')
- w2: bfloat16 [3072, 768], P('mp')
- w3: bfloat16 [768, 3072], P('mp')
- w4: bfloat16 [3072, 768], P('mp')
Outputs:
- output 1: float32 [768, 3072], P('mp')
- output 2: float32 [3072, 768], P('mp')
- output 3: float32 [768, 3072], P('mp')
- output 4: float32 [3072, 768], P('mp')
- output 5: bfloat16 [65536, 768], P(('mp', 'dpa', 'dpb', 'dpc'))
All inputs are finite; a program needn't handle non-finite values.
Results may differ from the reference program's by a relative error of at most 0.0114143.
Values are sent between devices in bfloat16 or wider.
A program may use at most 1 GiB of HBM per device.

```python
import jax
import jax.numpy as jnp
from jax import lax

D = 768
F = 3072
TOKENS_DEV = 8192
NDEV = 8
B = TOKENS_DEV * NDEV


def setup_inputs(seed: int = 0, part: int = 0) -> dict:
    key = jax.random.fold_in(jax.random.key(seed), part)
    ks = jax.random.split(key, 6)
    x = jax.random.normal(ks[0], (B, D), jnp.float32)
    g = jax.random.normal(ks[1], (B, D), jnp.float32)
    w1 = jax.random.normal(ks[2], (D, F), jnp.float32) * D ** -0.5
    w2 = jax.random.normal(ks[3], (F, D), jnp.float32) * F ** -0.5
    w3 = jax.random.normal(ks[4], (D, F), jnp.float32) * D ** -0.5
    w4 = jax.random.normal(ks[5], (F, D), jnp.float32) * F ** -0.5
    return {"x": x.astype(jnp.bfloat16), "g": g.astype(jnp.bfloat16), "w1": w1.astype(jnp.bfloat16), "w2": w2.astype(jnp.bfloat16), "w3": w3.astype(jnp.bfloat16), "w4": w4.astype(jnp.bfloat16)}


def gelu_grad(a, d):
    return jax.vjp(lambda t: jax.nn.gelu(t, approximate=True), a)[1](d)[0]


def block_grads(x, g, w1, w2, w3, w4):
    f32 = jnp.float32
    bf = jnp.bfloat16
    a1 = jnp.dot(x, w1, preferred_element_type=f32).astype(bf)
    h1 = jax.nn.gelu(a1.astype(f32), approximate=True).astype(bf)
    h2 = (jnp.dot(h1, w2, preferred_element_type=f32) + x.astype(f32)).astype(bf)
    a3 = jnp.dot(h2, w3, preferred_element_type=f32).astype(bf)
    h3 = jax.nn.gelu(a3.astype(f32), approximate=True).astype(bf)
    dw4 = jnp.dot(h3.T, g, preferred_element_type=f32)
    dh3 = jnp.dot(g, w4.T, preferred_element_type=f32).astype(bf)
    da3 = gelu_grad(a3.astype(f32), dh3.astype(f32)).astype(bf)
    dw3 = jnp.dot(h2.T, da3, preferred_element_type=f32)
    dh2 = (jnp.dot(da3, w3.T, preferred_element_type=f32) + g.astype(f32)).astype(bf)
    dw2 = jnp.dot(h1.T, dh2, preferred_element_type=f32)
    dh1 = jnp.dot(dh2, w2.T, preferred_element_type=f32).astype(bf)
    da1 = gelu_grad(a1.astype(f32), dh1.astype(f32)).astype(bf)
    dw1 = jnp.dot(x.T, da1, preferred_element_type=f32)
    dx = (jnp.dot(da1, w1.T, preferred_element_type=f32) + dh2.astype(f32)).astype(bf)
    return dw1, dw2, dw3, dw4, dx


def reference(x, g, w1, w2, w3, w4):
    xs = x.reshape(NDEV, TOKENS_DEV, D)
    gs = g.reshape(NDEV, TOKENS_DEV, D)

    def body(acc, xg):
        res = block_grads(xg[0], xg[1], w1, w2, w3, w4)
        acc = tuple(a + b for a, b in zip(acc, res[:4]))
        return acc, res[4]

    zero = (jnp.zeros((D, F), jnp.float32), jnp.zeros((F, D), jnp.float32), jnp.zeros((D, F), jnp.float32), jnp.zeros((F, D), jnp.float32))
    acc, dxs = lax.scan(body, zero, (xs, gs))
    return acc[0] / NDEV, acc[1] / NDEV, acc[2] / NDEV, acc[3] / NDEV, dxs.reshape(B, D)
```

```python
import functools
import jax, jax.numpy as jnp
from jax import lax
from jax.experimental import pallas as pl
from jax.experimental.pallas import tpu as pltpu
from jax.sharding import PartitionSpec as P
f32=jnp.float32; bf=jnp.bfloat16
D=768; F=3072; N=8192
C1=0.7978845608028654; C2=C1*0.044715
def nn(a,b): return lax.dot_general(a,b,(((1,),(0,)),((),())),preferred_element_type=f32)
def nt(a,b): return lax.dot_general(a,b,(((1,),(1,)),((),())),preferred_element_type=f32)
def tn(a,b): return lax.dot_general(a,b,(((0,),(0,)),((),())),preferred_element_type=f32)
def gelu_f(x):
    t=jnp.tanh(x*(C1+C2*(x*x)))
    return (0.5*x)*(1.0+t)
def gelu_both(x,d):
    x2=x*x
    t=jnp.tanh(x*(C1+C2*x2))
    s=1.0+t; hx=0.5*x
    w=((1.0-t)*s)*hx
    gp=0.5*s+w*(C1+(3.0*C2)*x2)
    return hx*s, gp*d
def k1(x_ref,w1_ref,w2_ref,a1_ref,h2_ref,h1_scr,*,sub,fch):
    R=x_ref.shape[0]
    for j in range(R//sub):
        sl=pl.ds(j*sub,sub)
        for f in range(F//fch):
            fs=pl.ds(f*fch,fch)
            a1_ref[sl,fs]=nn(x_ref[sl,:],w1_ref[:,fs]).astype(bf)
            h1_scr[sl,fs]=gelu_f(a1_ref[sl,fs].astype(f32)).astype(bf)
        h2_ref[sl,:]=(nn(h1_scr[sl,:],w2_ref[...])+x_ref[sl,:].astype(f32)).astype(bf)
def call_k1(x,w1,w2,R=512,sub=256,fch=768):
    return pl.pallas_call(functools.partial(k1,sub=sub,fch=fch),grid=(N//R,),
      in_specs=[pl.BlockSpec((R,D),lambda r:(r,0)),pl.BlockSpec((D,F),lambda r:(0,0)),pl.BlockSpec((F,D),lambda r:(0,0))],
      out_specs=[pl.BlockSpec((R,F),lambda r:(r,0)),pl.BlockSpec((R,D),lambda r:(r,0))],
      out_shape=[jax.ShapeDtypeStruct((N,F),bf),jax.ShapeDtypeStruct((N,D),bf)],
      scratch_shapes=[pltpu.VMEM((R,F),bf)],
      compiler_params=pltpu.CompilerParams(vmem_limit_bytes=60*2**20),name="k1",cost_estimate=pl.CostEstimate(flops=4*N*D*F,bytes_accessed=2*N*(F+2*D),transcendentals=N*F))(x,w1,w2)
def k2(h2_ref,g_ref,w3_ref,w4_ref,da3_ref,p3_ref,p4_ref,a_scr,d_scr,h_scr,*,sub):
    R=h2_ref.shape[0]; n=R//sub
    r=pl.program_id(1)
    @pl.when(r==0)
    def _():
        p3_ref[...]=jnp.zeros_like(p3_ref); p4_ref[...]=jnp.zeros_like(p4_ref)
    def dd(j):
        sl=pl.ds(j*sub,sub)
        a_scr[sl,:]=nn(h2_ref[sl,:],w3_ref[...]).astype(bf)
        d_scr[sl,:]=nt(g_ref[sl,:],w4_ref[...]).astype(bf)
    def ee(j):
        sl=pl.ds(j*sub,sub)
        h,da=gelu_both(a_scr[sl,:].astype(f32),d_scr[sl,:].astype(f32))
        h_scr[sl,:]=h.astype(bf); da3_ref[sl,:]=da.astype(bf)
    def pp(j):
        sl=pl.ds(j*sub,sub)
        p4_ref[...]+=tn(h_scr[sl,:],g_ref[sl,:])
        p3_ref[...]+=tn(h2_ref[sl,:],da3_ref[sl,:])
    for j in range(n):
        dd(j)
        if j>0: ee(j-1)
        if j>1: pp(j-2)
    ee(n-1)
    if n>1: pp(n-2)
    pp(n-1)
def call_k2(h2,g,w3,w4,R=1024,sub=512,fc=768):
    return pl.pallas_call(functools.partial(k2,sub=sub),grid=(F//fc,N//R),
      in_specs=[pl.BlockSpec((R,D),lambda c,r:(r,0)),pl.BlockSpec((R,D),lambda c,r:(r,0)),pl.BlockSpec((D,fc),lambda c,r:(0,c)),pl.BlockSpec((fc,D),lambda c,r:(c,0))],
      out_specs=[pl.BlockSpec((R,fc),lambda c,r:(r,c)),pl.BlockSpec((D,fc),lambda c,r:(0,c)),pl.BlockSpec((fc,D),lambda c,r:(c,0))],
      out_shape=[jax.ShapeDtypeStruct((N,F),bf),jax.ShapeDtypeStruct((D,F),f32),jax.ShapeDtypeStruct((F,D),f32)],
      scratch_shapes=[pltpu.VMEM((R,fc),bf)]*3,
      compiler_params=pltpu.CompilerParams(vmem_limit_bytes=60*2**20),name="k2",cost_estimate=pl.CostEstimate(flops=8*N*D*F,bytes_accessed=2*N*(F+8*D),transcendentals=N*F))(h2,g,w3,w4)
def k3(*refs,sub):
    *a_refs,w_ref,r_ref,o_ref=refs
    R=r_ref.shape[0]
    for j in range(R//sub):
        sl=pl.ds(j*sub,sub)
        acc=r_ref[sl,:].astype(f32)
        k=0
        for a_ref in a_refs:
            w=a_ref.shape[1]
            acc=nt(a_ref[sl,:],w_ref[:,k:k+w])+acc
            k+=w
        o_ref[sl,:]=acc.astype(bf)
def call_k3(parts,w,res,R=1024,sub=512):
    return pl.pallas_call(functools.partial(k3,sub=sub),grid=(N//R,),
      in_specs=[pl.BlockSpec((R,a.shape[1]),lambda r:(r,0)) for a in parts]+[pl.BlockSpec((D,F),lambda r:(0,0)),pl.BlockSpec((R,D),lambda r:(r,0))],
      out_specs=pl.BlockSpec((R,D),lambda r:(r,0)),out_shape=jax.ShapeDtypeStruct((N,D),bf),
      compiler_params=pltpu.CompilerParams(vmem_limit_bytes=60*2**20),name="k3",cost_estimate=pl.CostEstimate(flops=2*N*D*F,bytes_accessed=2*N*(F+2*D),transcendentals=0))(*parts,w,res)
def k4(x_ref,dh2_ref,a1_ref,w2_ref,da1_ref,p1_ref,p2_ref,d_scr,h_scr,*,sub):
    R=x_ref.shape[0]; n=R//sub
    r=pl.program_id(1)
    @pl.when(r==0)
    def _():
        p1_ref[...]=jnp.zeros_like(p1_ref); p2_ref[...]=jnp.zeros_like(p2_ref)
    def dd(j):
        sl=pl.ds(j*sub,sub)
        d_scr[sl,:]=nt(dh2_ref[sl,:],w2_ref[...]).astype(bf)
    def ee(j):
        sl=pl.ds(j*sub,sub)
        h,da=gelu_both(a1_ref[sl,:].astype(f32),d_scr[sl,:].astype(f32))
        h_scr[sl,:]=h.astype(bf); da1_ref[sl,:]=da.astype(bf)
    def pp(j):
        sl=pl.ds(j*sub,sub)
        p2_ref[...]+=tn(h_scr[sl,:],dh2_ref[sl,:])
        p1_ref[...]+=tn(x_ref[sl,:],da1_ref[sl,:])
    for j in range(n):
        dd(j)
        if j>0: ee(j-1)
        if j>1: pp(j-2)
    ee(n-1)
    if n>1: pp(n-2)
    pp(n-1)
def call_k4(x,dh2,a1,w2,c0,nc,R=1024,sub=512,fc=768):
    return pl.pallas_call(functools.partial(k4,sub=sub),grid=(nc,N//R),
      in_specs=[pl.BlockSpec((R,D),lambda c,r:(r,0)),pl.BlockSpec((R,D),lambda c,r:(r,0)),pl.BlockSpec((R,fc),lambda c,r:(r,c+c0)),pl.BlockSpec((fc,D),lambda c,r:(c+c0,0))],
      out_specs=[pl.BlockSpec((R,fc),lambda c,r:(r,c)),pl.BlockSpec((D,fc),lambda c,r:(0,c)),pl.BlockSpec((fc,D),lambda c,r:(c,0))],
      out_shape=[jax.ShapeDtypeStruct((N,nc*fc),bf),jax.ShapeDtypeStruct((D,nc*fc),f32),jax.ShapeDtypeStruct((nc*fc,D),f32)],
      scratch_shapes=[pltpu.VMEM((R,fc),bf)]*2,
      compiler_params=pltpu.CompilerParams(vmem_limit_bytes=60*2**20),name="k4",cost_estimate=pl.CostEstimate(flops=3*N*D*F,bytes_accessed=2*N*(2*F+8*D),transcendentals=N*F))(x,dh2,a1,w2)


def solution(mesh):
    ndev = mesh.shape["dpa"] * mesh.shape["dpb"] * mesh.shape["dpc"]
    rows = P(("mp", "dpa", "dpb", "dpc"), None)
    wspec = P("mp", None)
    group = ("dpa", "dpb", "dpc")

    def scatter(dw):
        return lax.psum_scatter(dw, group, scatter_dimension=0, tiled=True)

    def gather(s):
        return lax.all_gather(s, group, axis=0, tiled=True) / ndev

    def local(x, g, w1, w2, w3, w4):
        a1, h2 = call_k1(x, w1, w2, 512, 256)
        da3, p3, p4 = call_k2(h2, g, w3, w4, 1024, 256)
        s3, s4 = scatter(p3), scatter(p4)
        dh2 = call_k3([da3], w3, g, 1024, 512)
        da1a, p1a, p2a = call_k4(x, dh2, a1, w2, 0, 2)
        da1a, dh2b, s3, s4 = lax.optimization_barrier((da1a, dh2, s3, s4))
        dw3, dw4 = gather(s3), gather(s4)
        da1b, p1b, p2b = call_k4(x, dh2b, a1, w2, 2, 2)
        s1a, s2a, s1b, s2b = scatter(p1a), scatter(p2a), scatter(p1b), scatter(p2b)
        dx = call_k3([da1a, da1b], w1, dh2, 1024, 512)
        dw1 = jnp.concatenate([gather(s1a), gather(s1b)], axis=1)
        dw2 = jnp.concatenate([gather(s2a), gather(s2b)], axis=0)
        return dw1, dw2, dw3, dw4, dx

    return jax.shard_map(local, mesh=mesh, in_specs=(rows, rows, wspec, wspec, wspec, wspec), out_specs=(wspec, wspec, wspec, wspec, rows), check_vma=False)
```

```python
import functools

import jax
import jax.numpy as jnp
from jax import lax
from jax.experimental import pallas as pl
from jax.experimental.pallas import tpu as pltpu
from jax.sharding import PartitionSpec as P

f32 = jnp.float32
bf = jnp.bfloat16
D = 768
F = 3072
N = 8192
FC = 768
NC = F // FC
C1 = 0.7978845608028654
C2 = C1 * 0.044715
MESH = pl.DeviceIdType.MESH
HR, IR, JR = 384, 192, 96
VMEM_BYTES = 63 * 2**20


def nn(a, b):
    return lax.dot_general(a, b, (((1,), (0,)), ((), ())), preferred_element_type=f32)


def nt(a, b):
    return lax.dot_general(a, b, (((1,), (1,)), ((), ())), preferred_element_type=f32)


def tn(a, b):
    return lax.dot_general(a, b, (((0,), (0,)), ((), ())), preferred_element_type=f32)


def gelu_f(x):
    t = jnp.tanh(x * (C1 + C2 * (x * x)))
    return (0.5 * x) * (1.0 + t)


def gelu_both(x, d):
    x2 = x * x
    t = jnp.tanh(x * (C1 + C2 * x2))
    s = 1.0 + t
    hx = 0.5 * x
    w = ((1.0 - t) * s) * hx
    return hx * s, (0.5 * s + w * (C1 + (3.0 * C2) * x2)) * d


def k1(x_ref, w1_ref, w2_ref, a1_ref, h2_ref, h1_scr, *, sub, fch):
    for j in range(x_ref.shape[0] // sub):
        sl = pl.ds(j * sub, sub)
        for f in range(F // fch):
            fs = pl.ds(f * fch, fch)
            a1_ref[sl, fs] = nn(x_ref[sl, :], w1_ref[:, fs]).astype(bf)
            h1_scr[sl, fs] = gelu_f(a1_ref[sl, fs].astype(f32)).astype(bf)
        h2_ref[sl, :] = (nn(h1_scr[sl, :], w2_ref[...]) + x_ref[sl, :].astype(f32)).astype(bf)


def call_k1(x, w1, w2, R=512, sub=256, fch=768):
    return pl.pallas_call(
        functools.partial(k1, sub=sub, fch=fch),
        grid=(N // R,),
        in_specs=[pl.BlockSpec((R, D), lambda r: (r, 0)), pl.BlockSpec((D, F), lambda r: (0, 0)), pl.BlockSpec((F, D), lambda r: (0, 0))],
        out_specs=[pl.BlockSpec((R, F), lambda r: (r, 0)), pl.BlockSpec((R, D), lambda r: (r, 0))],
        out_shape=[jax.ShapeDtypeStruct((N, F), bf), jax.ShapeDtypeStruct((N, D), bf)],
        scratch_shapes=[pltpu.VMEM((R, F), bf)],
        compiler_params=pltpu.CompilerParams(vmem_limit_bytes=VMEM_BYTES),
        cost_estimate=pl.CostEstimate(flops=4 * N * D * F, bytes_accessed=2 * N * (F + 2 * D), transcendentals=N * F),
        name="k1",
    )(x, w1, w2)


def comm_scratch(slots):
    sem = pltpu.SemaphoreType.DMA
    return [
        pltpu.VMEM((slots, 2, FC, D), f32),
        pltpu.VMEM((2, FC, D), f32),
        pltpu.VMEM((2, 2, IR, D), f32),
        pltpu.VMEM((2, 2, JR, D), f32),
        pltpu.VMEM((2, FC, D), f32),
        sem((2, 2)),
        sem((4, 2, 2, 2)),
        sem((2, 3)),
        sem((2,)),
    ]


class Comm:
    def __init__(self, scr, red):
        self.acc, self.rx0, self.rx1, self.rx2, self.res, self.sem0, self.semx, self.sem5, self.seml = scr
        self.red = red
        self.a, self.b, self.c = lax.axis_index("dpa"), lax.axis_index("dpb"), lax.axis_index("dpc")
        self.mi, self.mj = (self.b, self.a), (self.a, self.b)
        x, y = {"dpb": 1 - self.b}, {"dpa": 1 - self.a}
        self.di, self.dj = (x, y), (y, x)
        self.dc = {"dpc": 1 - self.c}

    def barrier(self):
        sem = pltpu.get_barrier_semaphore()
        for dev in (self.di[0], self.di[1], self.dc):
            pl.semaphore_signal(sem, inc=1, device_id=dev, device_id_type=MESH)
        pl.semaphore_wait(sem, 3)

    def rows_i(self, h, i):
        return pl.ds(pl.multiple_of(h * HR + i * IR, JR), IR)

    def rows_j(self, h, i, j):
        return pl.ds(pl.multiple_of(h * HR + i * IR + j * JR, JR), JR)

    def p0(self, slot, aslot):
        return pltpu.make_async_remote_copy(self.acc.at[aslot, 1 - self.c], self.rx0.at[slot], self.sem0.at[slot, 0], self.sem0.at[slot, 1], device_id=self.dc, device_id_type=MESH)

    def px(self, phase, h, slot, aslot=None):
        i, j = self.mi[h], self.mj[h]
        if phase == 1:
            src, dst, dev = self.acc.at[aslot, self.c, self.rows_i(h, 1 - i)], self.rx1.at[slot, h], self.di[h]
        elif phase == 2:
            src, dst, dev = self.acc.at[aslot, self.c, self.rows_j(h, i, 1 - j)], self.rx2.at[slot, h], self.dj[h]
        elif phase == 3:
            src = dst = self.res.at[slot, self.rows_j(h, i, j)]
            dev = self.dj[h]
        else:
            src = dst = self.res.at[slot, self.rows_i(h, i)]
            dev = self.di[h]
        return pltpu.make_async_remote_copy(src, dst, self.semx.at[phase - 1, slot, h, 0], self.semx.at[phase - 1, slot, h, 1], device_id=dev, device_id_type=MESH)

    def p5(self, slot, idx):
        src, dst = self.res.at[slot], self.red.at[idx, self.c]
        return (
            pltpu.make_async_remote_copy(src, dst, self.sem5.at[slot, 0], self.sem5.at[slot, 1], device_id=self.dc, device_id_type=MESH),
            pltpu.make_async_copy(src, dst, self.sem5.at[slot, 2]),
        )

    def start0(self, slot, aslot):
        self.p0(slot, aslot).start()

    def start1(self, slot, aslot):
        self.p0(slot, aslot).wait()
        for h in range(2):
            sl = self.rows_i(h, 1 - self.mi[h])
            self.acc[aslot, self.c, sl, :] += self.rx0[slot, sl, :]
        for h in range(2):
            self.px(1, h, slot, aslot).start()
        for h in range(2):
            sl = self.rows_i(h, self.mi[h])
            self.acc[aslot, self.c, sl, :] += self.rx0[slot, sl, :]

    def start2(self, slot, aslot):
        for h in range(2):
            self.px(1, h, slot, aslot).wait()
        for h in range(2):
            sl = self.rows_i(h, self.mi[h])
            self.acc[aslot, self.c, sl, :] += self.rx1[slot, h]
        for h in range(2):
            self.px(2, h, slot, aslot).start()

    def start3(self, slot, aslot):
        for h in range(2):
            self.px(2, h, slot, aslot).wait()
        for h in range(2):
            sl = self.rows_j(h, self.mi[h], self.mj[h])
            self.res[slot, sl, :] = (self.acc[aslot, self.c, sl, :] + self.rx2[slot, h]) * 0.125
        for h in range(2):
            self.px(3, h, slot).start()

    def wait3(self, slot):
        for h in range(2):
            self.px(3, h, slot).wait()

    def start4(self, slot):
        for h in range(2):
            self.px(4, h, slot).start()

    def start5(self, slot, idx):
        for h in range(2):
            self.px(4, h, slot).wait()
        for cp in self.p5(slot, idx):
            cp.start()

    def wait5(self, slot, idx):
        for cp in self.p5(slot, idx):
            cp.wait()


def comm_steps(cm, c, s, ev, *, nseg, acc_in, res_in, slots):
    cur, fin = lax.rem(c + 1, 2), lax.rem(c, 2)
    aslot = cur if slots == 2 else 0
    nfin0 = 1 if res_in else 0
    idx = jnp.where(c == 0, 0, c - 2 + nfin0) if not acc_in else 0
    if acc_in:
        has_cur = has_fin = None
    else:
        has_cur = c >= 1
        has_fin = (c >= 2) | (c == 0) if res_in else c >= 2

    def at(step, cond, f):
        pred = s == step
        if cond is not None:
            pred = pred & cond
        pl.when(pred)(f)

    events = [
        (ev["s0"], has_cur, lambda: cm.start0(cur, aslot)),
        (ev["s4"], has_fin, lambda: cm.start4(fin)),
        (ev["s1"], has_cur, lambda: cm.start1(cur, aslot)),
        (ev["s5"], has_fin, lambda: cm.start5(fin, idx)),
        (ev["s2"], has_cur, lambda: cm.start2(cur, aslot)),
        (ev["w5"], has_fin, lambda: cm.wait5(fin, idx)),
        (ev["s3"], has_cur, lambda: cm.start3(cur, aslot)),
        (ev["w3"], has_cur, lambda: cm.wait3(cur)),
    ]
    for step, cond, f in sorted(events, key=lambda e: e[0]):
        at(step, cond, f)


def load(cm, acc_in, res_in):
    cps = []
    if acc_in is not None:
        cps.append(pltpu.make_async_copy(acc_in, cm.acc.at[0], cm.seml.at[0]))
    if res_in is not None:
        cps.append(pltpu.make_async_copy(res_in, cm.res.at[0], cm.seml.at[1]))
    for cp in cps:
        cp.start()
    for cp in cps:
        cp.wait()


def store(cm, acc_out, aslot, res_out, rslot):
    cps = []
    if acc_out is not None:
        cps.append(pltpu.make_async_copy(cm.acc.at[aslot], acc_out, cm.seml.at[0]))
    if res_out is not None:
        cps.append(pltpu.make_async_copy(cm.res.at[rslot], res_out, cm.seml.at[1]))
    for cp in cps:
        cp.start()
    for cp in cps:
        cp.wait()


EV = {"s0": 0, "s4": 0, "s1": 2, "s5": 6, "s2": 7, "w5": 8, "s3": 10, "w3": 13}


def accumulate(n, dd, ee, pp):
    for j in range(n):
        dd(j)
        if j > 0:
            ee(j - 1)
        if j > 1:
            pp(j - 2)
    ee(n - 1)
    if n > 1:
        pp(n - 2)
    pp(n - 1)


def k2(h2_ref, g_ref, w3_ref, w4_ref, da3_ref, red, acc_out, res_out, a_scr, d_scr, h_scr, *scr, sub, ev):
    c, s = pl.program_id(0), pl.program_id(1)
    cm = Comm(scr, red)
    acc = cm.acc
    pl.when((c == 0) & (s == 0))(cm.barrier)
    slot = lax.rem(c, 2)
    comm_steps(cm, c, s, ev, nseg=NC, acc_in=False, res_in=False, slots=2)

    @pl.when(s == 0)
    def _():
        acc[slot] = jnp.zeros(acc.shape[1:], f32)

    def dd(j):
        sl = pl.ds(j * sub, sub)
        a_scr[sl, :] = nn(h2_ref[sl, :], w3_ref[...]).astype(bf)
        d_scr[sl, :] = nt(g_ref[sl, :], w4_ref[...]).astype(bf)

    def ee(j):
        sl = pl.ds(j * sub, sub)
        h, da = gelu_both(a_scr[sl, :].astype(f32), d_scr[sl, :].astype(f32))
        h_scr[sl, :] = h.astype(bf)
        da3_ref[sl, :] = da.astype(bf)

    def pp(j):
        sl = pl.ds(j * sub, sub)
        acc[slot, 1] += tn(h_scr[sl, :], g_ref[sl, :])
        acc[slot, 0] += tn(h2_ref[sl, :], da3_ref[sl, :])

    accumulate(h2_ref.shape[0] // sub, dd, ee, pp)

    @pl.when((c == NC - 1) & (s == pl.num_programs(1) - 1))
    def _():
        store(cm, acc_out, (NC - 1) % 2, res_out, NC % 2)


def any_spec():
    return pl.BlockSpec(memory_space=pltpu.HBM)


def red_shape(n):
    return jax.ShapeDtypeStruct((n, 2, FC, D), f32)


ACC_SHAPE = jax.ShapeDtypeStruct((2, FC, D), f32)
RES_SHAPE = jax.ShapeDtypeStruct((FC, D), f32)


def params(cid):
    return pltpu.CompilerParams(vmem_limit_bytes=VMEM_BYTES, collective_id=cid, has_side_effects=True)


def call_k2(h2, g, w3, w4, R=512, sub=256):
    row = pl.BlockSpec((R, D), lambda c, r: (r, 0))
    return pl.pallas_call(
        functools.partial(k2, sub=sub, ev=EV),
        grid=(NC, N // R),
        in_specs=[row, row, pl.BlockSpec((D, FC), lambda c, r: (0, c)), pl.BlockSpec((FC, D), lambda c, r: (c, 0))],
        out_specs=[pl.BlockSpec((R, FC), lambda c, r: (r, c)), any_spec(), any_spec(), any_spec()],
        out_shape=[jax.ShapeDtypeStruct((N, F), bf), red_shape(2), ACC_SHAPE, RES_SHAPE],
        scratch_shapes=[pltpu.VMEM((R, FC), bf)] * 3 + comm_scratch(2),
        compiler_params=params(0),
        cost_estimate=pl.CostEstimate(flops=8 * N * D * F, bytes_accessed=2 * N * (F + 8 * D), transcendentals=N * F),
        name="k2",
    )(h2, g, w3, w4)


def k3(a_ref, w_ref, r_ref, acc_in, res_in, o_ref, red, *rest, sub, ev, last):
    res_out, scr = (None, rest) if last else (rest[0], rest[1:])
    s = pl.program_id(0)
    end = pl.num_programs(0) - 1
    cm = Comm(scr, red)

    @pl.when(s == 0)
    def _():
        load(cm, acc_in, res_in)
        cm.barrier()

    comm_steps(cm, 0, s, ev, nseg=1, acc_in=True, res_in=True, slots=1)
    for j in range(a_ref.shape[0] // sub):
        sl = pl.ds(j * sub, sub)
        o_ref[sl, :] = (nt(a_ref[sl, :], w_ref[...]) + r_ref[sl, :].astype(f32)).astype(bf)

    @pl.when(s == end)
    def _():
        if last:
            cm.start4(1)
            cm.start5(1, 1)
            cm.wait5(1, 1)
        else:
            store(cm, None, None, res_out, 1)


def call_k3(a, w, res, acc_in, res_in, last, cid, R=512, sub=256):
    row = pl.BlockSpec((R, D), lambda r: (r, 0))
    return pl.pallas_call(
        functools.partial(k3, sub=sub, ev=EV, last=last),
        grid=(N // R,),
        in_specs=[pl.BlockSpec((R, F), lambda r: (r, 0)), pl.BlockSpec((D, F), lambda r: (0, 0)), row, any_spec(), any_spec()],
        out_specs=[row, any_spec()] + ([] if last else [any_spec()]),
        out_shape=[jax.ShapeDtypeStruct((N, D), bf), red_shape(2 if last else 1)] + ([] if last else [RES_SHAPE]),
        scratch_shapes=comm_scratch(1),
        compiler_params=params(cid),
        cost_estimate=pl.CostEstimate(flops=2 * N * D * F, bytes_accessed=2 * N * (F + 2 * D), transcendentals=0),
        name="k5" if last else "k3",
    )(a, w, res, acc_in, res_in)


def k4(x_ref, dh2_ref, a1_ref, w2_ref, res_in, da1_ref, red, acc_out, res_out, d_scr, h_scr, *scr, sub, ev):
    c, s = pl.program_id(0), pl.program_id(1)
    cm = Comm(scr, red)
    acc = cm.acc

    @pl.when((c == 0) & (s == 0))
    def _():
        load(cm, None, res_in)
        cm.barrier()

    slot = lax.rem(c, 2)
    comm_steps(cm, c, s, ev, nseg=NC, acc_in=False, res_in=True, slots=2)

    @pl.when(s == 0)
    def _():
        acc[slot] = jnp.zeros(acc.shape[1:], f32)

    def dd(j):
        sl = pl.ds(j * sub, sub)
        d_scr[sl, :] = nt(dh2_ref[sl, :], w2_ref[...]).astype(bf)

    def ee(j):
        sl = pl.ds(j * sub, sub)
        h, da = gelu_both(a1_ref[sl, :].astype(f32), d_scr[sl, :].astype(f32))
        h_scr[sl, :] = h.astype(bf)
        da1_ref[sl, :] = da.astype(bf)

    def pp(j):
        sl = pl.ds(j * sub, sub)
        acc[slot, 1] += tn(h_scr[sl, :], dh2_ref[sl, :])
        acc[slot, 0] += tn(x_ref[sl, :], da1_ref[sl, :])

    accumulate(x_ref.shape[0] // sub, dd, ee, pp)

    @pl.when((c == NC - 1) & (s == pl.num_programs(1) - 1))
    def _():
        store(cm, acc_out, (NC - 1) % 2, res_out, NC % 2)


def call_k4(x, dh2, a1, w2, res_in, R=512, sub=256):
    row = pl.BlockSpec((R, D), lambda c, r: (r, 0))
    blk = pl.BlockSpec((R, FC), lambda c, r: (r, c))
    return pl.pallas_call(
        functools.partial(k4, sub=sub, ev=EV),
        grid=(NC, N // R),
        in_specs=[row, row, blk, pl.BlockSpec((FC, D), lambda c, r: (c, 0)), any_spec()],
        out_specs=[blk, any_spec(), any_spec(), any_spec()],
        out_shape=[jax.ShapeDtypeStruct((N, F), bf), red_shape(3), ACC_SHAPE, RES_SHAPE],
        scratch_shapes=[pltpu.VMEM((R, FC), bf)] * 2 + comm_scratch(2),
        compiler_params=params(2),
        cost_estimate=pl.CostEstimate(flops=6 * N * D * F, bytes_accessed=2 * N * (2 * F + 8 * D), transcendentals=N * F),
        name="k4",
    )(x, dh2, a1, w2, res_in)


def place(r2, r3, r4a, r4b, r5, dx_in, dw1, dw2, dw3, dw4, dx):
    c = pl.program_id(0) // 4
    dx[...] = dx_in[...]

    def put(cond, src, wa, wb):
        @pl.when(cond)
        def _():
            wa[...] = src[0, 0]
            wb[...] = src[0, 1]

    put(c < 2, r2, dw3, dw4)
    put(c == 2, r3, dw3, dw4)
    put(c == 3, r4a, dw3, dw4)
    put(c < 2, r4b, dw1, dw2)
    put(c >= 2, r5, dw1, dw2)


def call_place(r2, r3, r4, r5, dx):
    rows = FC // 4

    def spec(lo, n, first):
        def index(t):
            k = jnp.clip(t, 4 * lo, 4 * (lo + n) - 1)
            return first + k // 4 - lo, 0, lax.rem(k, 4), 0

        return pl.BlockSpec((1, 2, rows, D), index)

    row = pl.BlockSpec((N // 16, D), lambda t: (t, 0))
    wide = pl.BlockSpec((rows, FC), lambda t: (lax.rem(t, 4), t // 4))
    tall = pl.BlockSpec((rows, D), lambda t: (t, 0))
    return pl.pallas_call(
        place,
        grid=(16,),
        in_specs=[spec(0, 2, 0), spec(2, 1, 0), spec(3, 1, 0), spec(0, 2, 1), spec(2, 2, 0), row],
        out_specs=[wide, tall, wide, tall, row],
        out_shape=[jax.ShapeDtypeStruct((D, F), f32), jax.ShapeDtypeStruct((F, D), f32)] * 2 + [jax.ShapeDtypeStruct((N, D), bf)],
        compiler_params=pltpu.CompilerParams(vmem_limit_bytes=VMEM_BYTES),
        name="place",
    )(r2, r3, r4, r4, r5, dx)


def solution(mesh):
    rows = P(("mp", "dpa", "dpb", "dpc"), None)
    wspec = P("mp", None)

    def local(x, g, w1, w2, w3, w4):
        a1, h2 = call_k1(x, w1, w2)
        da3, r2, acc, res = call_k2(h2, g, w3, w4)
        dh2, r3, res = call_k3(da3, w3, g, acc, res, False, 1)
        da1, r4, acc, res = call_k4(x, dh2, a1, w2, res)
        dx, r5 = call_k3(da1, w1, dh2, acc, res, True, 3)
        return tuple(call_place(r2, r3, r4, r5, dx))

    return jax.shard_map(local, mesh=mesh, in_specs=(rows, rows, wspec, wspec, wspec, wspec), out_specs=(wspec, wspec, wspec, wspec, rows), check_vma=False)
```

```python
import functools

import jax
import jax.numpy as jnp
from jax import lax
from jax.experimental import pallas as pl
from jax.experimental.pallas import tpu as pltpu
from jax.sharding import PartitionSpec as P

f32 = jnp.float32
bf = jnp.bfloat16
D = 768
F = 3072
N = 8192
FC = 768
NC = F // FC
C1 = 0.7978845608028654
C2 = C1 * 0.044715
MESH = pl.DeviceIdType.MESH
HR, IR, JR = 384, 192, 96
VMEM_BYTES = 63 * 2**20


def nn(a, b):
    return lax.dot_general(a, b, (((1,), (0,)), ((), ())), preferred_element_type=f32)


def nt(a, b):
    return lax.dot_general(a, b, (((1,), (1,)), ((), ())), preferred_element_type=f32)


def tn(a, b):
    return lax.dot_general(a, b, (((0,), (0,)), ((), ())), preferred_element_type=f32)


def gelu_f(x):
    t = jnp.tanh(x * (C1 + C2 * (x * x)))
    return (0.5 * x) * (1.0 + t)


def gelu_both(x, d):
    x2 = x * x
    t = jnp.tanh(x * (C1 + C2 * x2))
    s = 1.0 + t
    hx = 0.5 * x
    w = ((1.0 - t) * s) * hx
    return hx * s, (0.5 * s + w * (C1 + (3.0 * C2) * x2)) * d


def k1(x_ref, w1_ref, w2_ref, a1_ref, h2_ref, h1_scr, *, sub, fch):
    for j in range(x_ref.shape[0] // sub):
        sl = pl.ds(j * sub, sub)
        for f in range(F // fch):
            fs = pl.ds(f * fch, fch)
            a1_ref[sl, fs] = nn(x_ref[sl, :], w1_ref[:, fs]).astype(bf)
            h1_scr[sl, fs] = gelu_f(a1_ref[sl, fs].astype(f32)).astype(bf)
        h2_ref[sl, :] = (nn(h1_scr[sl, :], w2_ref[...]) + x_ref[sl, :].astype(f32)).astype(bf)


def call_k1(x, w1, w2, R=1024, sub=256, fch=768):
    return pl.pallas_call(
        functools.partial(k1, sub=sub, fch=fch),
        grid=(N // R,),
        in_specs=[pl.BlockSpec((R, D), lambda r: (r, 0)), pl.BlockSpec((D, F), lambda r: (0, 0)), pl.BlockSpec((F, D), lambda r: (0, 0))],
        out_specs=[pl.BlockSpec((R, F), lambda r: (r, 0)), pl.BlockSpec((R, D), lambda r: (r, 0))],
        out_shape=[jax.ShapeDtypeStruct((N, F), bf), jax.ShapeDtypeStruct((N, D), bf)],
        scratch_shapes=[pltpu.VMEM((R, F), bf)],
        compiler_params=pltpu.CompilerParams(vmem_limit_bytes=VMEM_BYTES),
        cost_estimate=pl.CostEstimate(flops=4 * N * D * F, bytes_accessed=2 * N * (F + 2 * D), transcendentals=N * F),
        name="k1",
    )(x, w1, w2)


def comm_scratch(slots):
    sem = pltpu.SemaphoreType.DMA
    return [
        pltpu.VMEM((slots, 2, FC, D), f32),
        pltpu.VMEM((2, FC, D), f32),
        pltpu.VMEM((2, 2, IR, D), f32),
        pltpu.VMEM((2, 2, JR, D), f32),
        pltpu.VMEM((2, FC, D), f32),
        sem((2, 2)),
        sem((4, 2, 2, 2)),
        sem((2, 3)),
        sem((2,)),
    ]


class Comm:
    def __init__(self, scr, red):
        self.acc, self.rx0, self.rx1, self.rx2, self.res, self.sem0, self.semx, self.sem5, self.seml = scr
        self.red = red
        self.a, self.b, self.c = lax.axis_index("dpa"), lax.axis_index("dpb"), lax.axis_index("dpc")
        self.mi, self.mj = (self.b, self.a), (self.a, self.b)
        x, y = {"dpb": 1 - self.b}, {"dpa": 1 - self.a}
        self.di, self.dj = (x, y), (y, x)
        self.dc = {"dpc": 1 - self.c}

    def barrier(self):
        sem = pltpu.get_barrier_semaphore()
        for dev in (self.di[0], self.di[1], self.dc):
            pl.semaphore_signal(sem, inc=1, device_id=dev, device_id_type=MESH)
        pl.semaphore_wait(sem, 3)

    def rows_i(self, h, i):
        return pl.ds(pl.multiple_of(h * HR + i * IR, JR), IR)

    def rows_j(self, h, i, j):
        return pl.ds(pl.multiple_of(h * HR + i * IR + j * JR, JR), JR)

    def p0(self, slot, aslot):
        return pltpu.make_async_remote_copy(self.acc.at[aslot, 1 - self.c], self.rx0.at[slot], self.sem0.at[slot, 0], self.sem0.at[slot, 1], device_id=self.dc, device_id_type=MESH)

    def px(self, phase, h, slot, aslot=None):
        i, j = self.mi[h], self.mj[h]
        if phase == 1:
            src, dst, dev = self.acc.at[aslot, self.c, self.rows_i(h, 1 - i)], self.rx1.at[slot, h], self.di[h]
        elif phase == 2:
            src, dst, dev = self.acc.at[aslot, self.c, self.rows_j(h, i, 1 - j)], self.rx2.at[slot, h], self.dj[h]
        elif phase == 3:
            src = dst = self.res.at[slot, self.rows_j(h, i, j)]
            dev = self.dj[h]
        else:
            src = dst = self.res.at[slot, self.rows_i(h, i)]
            dev = self.di[h]
        return pltpu.make_async_remote_copy(src, dst, self.semx.at[phase - 1, slot, h, 0], self.semx.at[phase - 1, slot, h, 1], device_id=dev, device_id_type=MESH)

    def p5(self, slot, idx):
        src, dst = self.res.at[slot], self.red.at[idx, self.c]
        return (
            pltpu.make_async_remote_copy(src, dst, self.sem5.at[slot, 0], self.sem5.at[slot, 1], device_id=self.dc, device_id_type=MESH),
            pltpu.make_async_copy(src, dst, self.sem5.at[slot, 2]),
        )

    def start0(self, slot, aslot):
        self.p0(slot, aslot).start()

    def start1(self, slot, aslot):
        self.p0(slot, aslot).wait()
        for h in range(2):
            sl = self.rows_i(h, 1 - self.mi[h])
            self.acc[aslot, self.c, sl, :] += self.rx0[slot, sl, :]
        for h in range(2):
            self.px(1, h, slot, aslot).start()
        for h in range(2):
            sl = self.rows_i(h, self.mi[h])
            self.acc[aslot, self.c, sl, :] += self.rx0[slot, sl, :]

    def start2(self, slot, aslot):
        for h in range(2):
            self.px(1, h, slot, aslot).wait()
        for h in range(2):
            sl = self.rows_i(h, self.mi[h])
            self.acc[aslot, self.c, sl, :] += self.rx1[slot, h]
        for h in range(2):
            self.px(2, h, slot, aslot).start()

    def end2(self, slot, aslot):
        for h in range(2):
            self.px(2, h, slot, aslot).wait()
        for h in range(2):
            sl = self.rows_j(h, self.mi[h], self.mj[h])
            self.res[slot, sl, :] = (self.acc[aslot, self.c, sl, :] + self.rx2[slot, h]) * 0.125

    def start3(self, slot):
        for h in range(2):
            self.px(3, h, slot).start()

    def start4(self, slot):
        for h in range(2):
            self.px(3, h, slot).wait()
        for h in range(2):
            self.px(4, h, slot).start()

    def start5(self, slot, idx):
        for h in range(2):
            self.px(4, h, slot).wait()
        for cp in self.p5(slot, idx):
            cp.start()

    def wait5(self, slot, idx):
        for cp in self.p5(slot, idx):
            cp.wait()


def comm_steps(cm, c, t, ev, *, acc_in, res_in, slots, end=False):
    cur, fin = lax.rem(c + 1, 2), lax.rem(c, 2)
    aslot = cur if slots == 2 else 0
    if acc_in:
        has_cur = has_fin = None
        idx = 0
    else:
        has_cur = c >= 1
        has_fin = (c >= 2) | (c == 0) if res_in else c >= 2
        idx = jnp.where(c == 0, 0, c - 1) if res_in else jnp.maximum(c - 2, 0)
    events = [
        ("s0", has_cur, lambda: cm.start0(cur, aslot)),
        ("s3", has_fin, lambda: cm.start3(fin)),
        ("s1", has_cur, lambda: cm.start1(cur, aslot)),
        ("s4", has_fin, lambda: cm.start4(fin)),
        ("s2", has_cur, lambda: cm.start2(cur, aslot)),
        ("s5", has_fin, lambda: cm.start5(fin, idx)),
        ("w5", has_fin, lambda: cm.wait5(fin, idx)),
        ("e2", has_cur, lambda: cm.end2(cur, aslot)),
    ]
    for key, cond, f in sorted(events, key=lambda e: ev[e[0]]):
        if (ev[key] >= SLOTS) != end:
            continue
        pred = t == (SLOTS - 1 if end else ev[key])
        pl.when(pred if cond is None else pred & cond)(f)


def load(cm, acc_in, res_in):
    cps = []
    if acc_in is not None:
        cps.append(pltpu.make_async_copy(acc_in, cm.acc.at[0], cm.seml.at[0]))
    if res_in is not None:
        cps.append(pltpu.make_async_copy(res_in, cm.res.at[0], cm.seml.at[1]))
    for cp in cps:
        cp.start()
    for cp in cps:
        cp.wait()


def store(cm, acc_out, aslot, res_out, rslot):
    cps = []
    if acc_out is not None:
        cps.append(pltpu.make_async_copy(cm.acc.at[aslot], acc_out, cm.seml.at[0]))
    if res_out is not None:
        cps.append(pltpu.make_async_copy(cm.res.at[rslot], res_out, cm.seml.at[1]))
    for cp in cps:
        cp.start()
    for cp in cps:
        cp.wait()


SLOTS = 8
SR = N // SLOTS
EV = {"s0": 0, "s3": 0, "s1": 1, "s4": 2, "s2": 5, "s5": 6, "w5": 7, "e2": 8}
EV4 = {"s0": 0, "s3": 0, "s1": 1, "s4": 2, "s2": 6, "s5": 7, "w5": 8, "e2": 8}
EV5 = {"s0": 0, "s3": 0, "s1": 1, "s4": 2, "s2": 5, "s5": 6, "w5": 7, "e2": 7}


def slots_of(rows, body):
    n = rows // SR

    def one(i, carry):
        body(i, pl.multiple_of(i * SR, SR))
        return carry

    if n == 1:
        body(0, 0)
    else:
        lax.fori_loop(0, n, one, 0)


def accumulate(n, dd, ee, pp):
    for j in range(n):
        dd(j)
        if j > 0:
            ee(j - 1)
        if j > 1:
            pp(j - 2)
    ee(n - 1)
    if n > 1:
        pp(n - 2)
    pp(n - 1)


def k2(h2_ref, g_ref, w3_ref, w4_ref, da3_ref, red, acc_out, res_out, a_scr, d_scr, h_scr, *scr, sub, ev):
    c, s = pl.program_id(0), pl.program_id(1)
    cm = Comm(scr, red)
    acc = cm.acc
    pl.when((c == 0) & (s == 0))(cm.barrier)
    slot = lax.rem(c, 2)
    n = h2_ref.shape[0] // SR

    def body(i, r0):
        t = s * n + i
        comm_steps(cm, c, t, ev, acc_in=False, res_in=False, slots=2)

        @pl.when(t == 0)
        def _():
            acc[slot] = jnp.zeros(acc.shape[1:], f32)

        def dd(j):
            sl, ss = pl.ds(r0 + j * sub, sub), pl.ds(j * sub, sub)
            a_scr[ss, :] = nn(h2_ref[sl, :], w3_ref[...]).astype(bf)
            d_scr[ss, :] = nt(g_ref[sl, :], w4_ref[...]).astype(bf)

        def ee(j):
            sl, ss = pl.ds(r0 + j * sub, sub), pl.ds(j * sub, sub)
            h, da = gelu_both(a_scr[ss, :].astype(f32), d_scr[ss, :].astype(f32))
            h_scr[ss, :] = h.astype(bf)
            da3_ref[sl, :] = da.astype(bf)

        def pp(j):
            sl, ss = pl.ds(r0 + j * sub, sub), pl.ds(j * sub, sub)
            acc[slot, 1] += tn(h_scr[ss, :], g_ref[sl, :])
            acc[slot, 0] += tn(h2_ref[sl, :], da3_ref[sl, :])

        accumulate(SR // sub, dd, ee, pp)
        comm_steps(cm, c, t, ev, acc_in=False, res_in=False, slots=2, end=True)

    slots_of(h2_ref.shape[0], body)

    @pl.when((c == NC - 1) & (s == pl.num_programs(1) - 1))
    def _():
        store(cm, acc_out, (NC - 1) % 2, res_out, NC % 2)


def any_spec():
    return pl.BlockSpec(memory_space=pltpu.HBM)


def red_shape(n):
    return jax.ShapeDtypeStruct((n, 2, FC, D), f32)


ACC_SHAPE = jax.ShapeDtypeStruct((2, FC, D), f32)
RES_SHAPE = jax.ShapeDtypeStruct((FC, D), f32)


def params(cid):
    return pltpu.CompilerParams(vmem_limit_bytes=VMEM_BYTES, collective_id=cid, has_side_effects=True)


def call_k2(h2, g, w3, w4, R=1024, sub=256):
    row = pl.BlockSpec((R, D), lambda c, r: (r, 0))
    return pl.pallas_call(
        functools.partial(k2, sub=sub, ev=EV),
        grid=(NC, N // R),
        in_specs=[row, row, pl.BlockSpec((D, FC), lambda c, r: (0, c)), pl.BlockSpec((FC, D), lambda c, r: (c, 0))],
        out_specs=[pl.BlockSpec((R, FC), lambda c, r: (r, c)), any_spec(), any_spec(), any_spec()],
        out_shape=[jax.ShapeDtypeStruct((N, F), bf), red_shape(2), ACC_SHAPE, RES_SHAPE],
        scratch_shapes=[pltpu.VMEM((SR, FC), bf)] * 3 + comm_scratch(2),
        compiler_params=params(0),
        cost_estimate=pl.CostEstimate(flops=8 * N * D * F, bytes_accessed=2 * N * (F + 8 * D), transcendentals=N * F),
        name="k2",
    )(h2, g, w3, w4)


def k3(a_ref, w_ref, r_ref, acc_in, res_in, o_ref, red, *rest, sub, ev, last):
    res_out, scr = (None, rest) if last else (rest[0], rest[1:])
    s = pl.program_id(0)
    cm = Comm(scr, red)

    @pl.when(s == 0)
    def _():
        load(cm, acc_in, res_in)
        cm.barrier()

    n = a_ref.shape[0] // SR

    def body(i, r0):
        t = s * n + i
        comm_steps(cm, 0, t, ev, acc_in=True, res_in=True, slots=1)
        if last:
            pl.when(t == ev["e2"])(lambda: cm.start3(1))
        for j in range(SR // sub):
            sl = pl.ds(r0 + j * sub, sub)
            o_ref[sl, :] = (nt(a_ref[sl, :], w_ref[...]) + r_ref[sl, :].astype(f32)).astype(bf)
        comm_steps(cm, 0, t, ev, acc_in=True, res_in=True, slots=1, end=True)

    slots_of(a_ref.shape[0], body)

    @pl.when(s == pl.num_programs(0) - 1)
    def _():
        if last:
            cm.start4(1)
            cm.start5(1, 1)
            cm.wait5(1, 1)
        else:
            store(cm, None, None, res_out, 1)


def call_k3(a, w, res, acc_in, res_in, last, cid, R=1024, sub=512):
    row = pl.BlockSpec((R, D), lambda r: (r, 0))
    return pl.pallas_call(
        functools.partial(k3, sub=sub, ev=EV5 if last else EV, last=last),
        grid=(N // R,),
        in_specs=[pl.BlockSpec((R, F), lambda r: (r, 0)), pl.BlockSpec((D, F), lambda r: (0, 0)), row, any_spec(), any_spec()],
        out_specs=[row, any_spec()] + ([] if last else [any_spec()]),
        out_shape=[jax.ShapeDtypeStruct((N, D), bf), red_shape(2 if last else 1)] + ([] if last else [RES_SHAPE]),
        scratch_shapes=comm_scratch(1),
        compiler_params=params(cid),
        cost_estimate=pl.CostEstimate(flops=2 * N * D * F, bytes_accessed=2 * N * (F + 2 * D), transcendentals=0),
        name="k5" if last else "k3",
    )(a, w, res, acc_in, res_in)


def k4(x_ref, dh2_ref, a1_ref, w2_ref, res_in, da1_ref, red, acc_out, res_out, d_scr, h_scr, *scr, sub, ev):
    c, s = pl.program_id(0), pl.program_id(1)
    cm = Comm(scr, red)
    acc = cm.acc

    @pl.when((c == 0) & (s == 0))
    def _():
        load(cm, None, res_in)
        cm.barrier()

    slot = lax.rem(c, 2)
    n = x_ref.shape[0] // SR

    def body(i, r0):
        t = s * n + i
        comm_steps(cm, c, t, ev, acc_in=False, res_in=True, slots=2)

        @pl.when(t == 0)
        def _():
            acc[slot] = jnp.zeros(acc.shape[1:], f32)

        def dd(j):
            sl, ss = pl.ds(r0 + j * sub, sub), pl.ds(j * sub, sub)
            d_scr[ss, :] = nt(dh2_ref[sl, :], w2_ref[...]).astype(bf)

        def ee(j):
            sl, ss = pl.ds(r0 + j * sub, sub), pl.ds(j * sub, sub)
            h, da = gelu_both(a1_ref[sl, :].astype(f32), d_scr[ss, :].astype(f32))
            h_scr[ss, :] = h.astype(bf)
            da1_ref[sl, :] = da.astype(bf)

        def pp(j):
            sl, ss = pl.ds(r0 + j * sub, sub), pl.ds(j * sub, sub)
            acc[slot, 1] += tn(h_scr[ss, :], dh2_ref[sl, :])
            acc[slot, 0] += tn(x_ref[sl, :], da1_ref[sl, :])

        accumulate(SR // sub, dd, ee, pp)
        comm_steps(cm, c, t, ev, acc_in=False, res_in=True, slots=2, end=True)

    slots_of(x_ref.shape[0], body)

    @pl.when((c == NC - 1) & (s == pl.num_programs(1) - 1))
    def _():
        store(cm, acc_out, (NC - 1) % 2, res_out, NC % 2)


def call_k4(x, dh2, a1, w2, res_in, R=1024, sub=512):
    row = pl.BlockSpec((R, D), lambda c, r: (r, 0))
    blk = pl.BlockSpec((R, FC), lambda c, r: (r, c))
    return pl.pallas_call(
        functools.partial(k4, sub=sub, ev=EV4),
        grid=(NC, N // R),
        in_specs=[row, row, blk, pl.BlockSpec((FC, D), lambda c, r: (c, 0)), any_spec()],
        out_specs=[blk, any_spec(), any_spec(), any_spec()],
        out_shape=[jax.ShapeDtypeStruct((N, F), bf), red_shape(3), ACC_SHAPE, RES_SHAPE],
        scratch_shapes=[pltpu.VMEM((SR, FC), bf)] * 2 + comm_scratch(2),
        compiler_params=params(2),
        cost_estimate=pl.CostEstimate(flops=6 * N * D * F, bytes_accessed=2 * N * (2 * F + 8 * D), transcendentals=N * F),
        name="k4",
    )(x, dh2, a1, w2, res_in)


def place(r2, r3, r4a, r4b, r5, dx_in, dw1, dw2, dw3, dw4, dx):
    c = pl.program_id(0) // 4
    dx[...] = dx_in[...]

    def put(cond, src, wa, wb):
        @pl.when(cond)
        def _():
            wa[...] = src[0, 0]
            wb[...] = src[0, 1]

    put(c < 2, r2, dw3, dw4)
    put(c == 2, r3, dw3, dw4)
    put(c == 3, r4a, dw3, dw4)
    put(c < 2, r4b, dw1, dw2)
    put(c >= 2, r5, dw1, dw2)


def call_place(r2, r3, r4, r5, dx):
    rows = FC // 4

    def spec(lo, n, first):
        def index(t):
            k = jnp.clip(t, 4 * lo, 4 * (lo + n) - 1)
            return first + k // 4 - lo, 0, lax.rem(k, 4), 0

        return pl.BlockSpec((1, 2, rows, D), index)

    row = pl.BlockSpec((N // 16, D), lambda t: (t, 0))
    wide = pl.BlockSpec((rows, FC), lambda t: (lax.rem(t, 4), t // 4))
    tall = pl.BlockSpec((rows, D), lambda t: (t, 0))
    return pl.pallas_call(
        place,
        grid=(16,),
        in_specs=[spec(0, 2, 0), spec(2, 1, 0), spec(3, 1, 0), spec(0, 2, 1), spec(2, 2, 0), row],
        out_specs=[wide, tall, wide, tall, row],
        out_shape=[jax.ShapeDtypeStruct((D, F), f32), jax.ShapeDtypeStruct((F, D), f32)] * 2 + [jax.ShapeDtypeStruct((N, D), bf)],
        compiler_params=pltpu.CompilerParams(vmem_limit_bytes=VMEM_BYTES),
        name="place",
    )(r2, r3, r4, r4, r5, dx)


def solution(mesh):
    rows = P(("mp", "dpa", "dpb", "dpc"), None)
    wspec = P("mp", None)

    def local(x, g, w1, w2, w3, w4):
        a1, h2 = call_k1(x, w1, w2)
        da3, r2, acc, res = call_k2(h2, g, w3, w4)
        dh2, r3, res = call_k3(da3, w3, g, acc, res, False, 1)
        da1, r4, acc, res = call_k4(x, dh2, a1, w2, res)
        dx, r5 = call_k3(da1, w1, dh2, acc, res, True, 3)
        return tuple(call_place(r2, r3, r4, r5, dx))

    return jax.shard_map(local, mesh=mesh, in_specs=(rows, rows, wspec, wspec, wspec, wspec), out_specs=(wspec, wspec, wspec, wspec, rows), check_vma=False)
```

```python
import functools

import jax
import jax.numpy as jnp
from jax import lax
from jax.experimental import pallas as pl
from jax.experimental.pallas import tpu as pltpu
from jax.sharding import PartitionSpec as P

f32 = jnp.float32
bf = jnp.bfloat16
D = 768
F = 3072
N = 8192
FC = 768
NC = F // FC
C1 = 0.7978845608028654
C2 = C1 * 0.044715
MESH = pl.DeviceIdType.MESH
HR, IR, JR = 384, 192, 96
VMEM_BYTES = 63 * 2**20


def nn(a, b):
    return lax.dot_general(a, b, (((1,), (0,)), ((), ())), preferred_element_type=f32)


def nt(a, b):
    return lax.dot_general(a, b, (((1,), (1,)), ((), ())), preferred_element_type=f32)


def tn(a, b):
    return lax.dot_general(a, b, (((0,), (0,)), ((), ())), preferred_element_type=f32)


def gelu_f(x):
    t = jnp.tanh(x * (C1 + C2 * (x * x)))
    return (0.5 * x) * (1.0 + t)


def gelu_both(x, d):
    x2 = x * x
    t = jnp.tanh(x * (C1 + C2 * x2))
    cdf = 0.5 + 0.5 * t
    h = x * cdf
    return h, (cdf + (h * (1.0 - t)) * (C1 + (3.0 * C2) * x2)) * d


def k1(x_ref, w1_ref, w2_ref, a1_ref, h2_ref, h1_scr, *, sub, fch):
    for j in range(x_ref.shape[0] // sub):
        sl = pl.ds(j * sub, sub)
        for f in range(F // fch):
            fs = pl.ds(f * fch, fch)
            a1_ref[sl, fs] = nn(x_ref[sl, :], w1_ref[:, fs]).astype(bf)
            h1_scr[sl, fs] = gelu_f(a1_ref[sl, fs].astype(f32)).astype(bf)
        h2_ref[sl, :] = (nn(h1_scr[sl, :], w2_ref[...]) + x_ref[sl, :].astype(f32)).astype(bf)


def call_k1(x, w1, w2, R=1024, sub=256, fch=768):
    return pl.pallas_call(
        functools.partial(k1, sub=sub, fch=fch),
        grid=(N // R,),
        in_specs=[pl.BlockSpec((R, D), lambda r: (r, 0)), pl.BlockSpec((D, F), lambda r: (0, 0)), pl.BlockSpec((F, D), lambda r: (0, 0))],
        out_specs=[pl.BlockSpec((R, F), lambda r: (r, 0)), pl.BlockSpec((R, D), lambda r: (r, 0))],
        out_shape=[jax.ShapeDtypeStruct((N, F), bf), jax.ShapeDtypeStruct((N, D), bf)],
        scratch_shapes=[pltpu.VMEM((R, F), bf)],
        compiler_params=pltpu.CompilerParams(vmem_limit_bytes=VMEM_BYTES),
        cost_estimate=pl.CostEstimate(flops=4 * N * D * F, bytes_accessed=2 * N * (F + 2 * D), transcendentals=N * F),
        name="k1",
    )(x, w1, w2)


def comm_scratch(slots):
    sem = pltpu.SemaphoreType.DMA
    return [
        pltpu.VMEM((slots, 2, FC, D), f32),
        pltpu.VMEM((2, FC, D), f32),
        pltpu.VMEM((2, 2, IR, D), f32),
        pltpu.VMEM((2, 2, JR, D), f32),
        pltpu.VMEM((2, FC, D), f32),
        sem((2, 2)),
        sem((4, 2, 2, 2)),
        sem((2, 3)),
        sem((2,)),
    ]


class Comm:
    def __init__(self, scr, red):
        self.acc, self.rx0, self.rx1, self.rx2, self.res, self.sem0, self.semx, self.sem5, self.seml = scr
        self.red = red
        self.a, self.b, self.c = lax.axis_index("dpa"), lax.axis_index("dpb"), lax.axis_index("dpc")
        self.mi, self.mj = (self.b, self.a), (self.a, self.b)
        x, y = {"dpb": 1 - self.b}, {"dpa": 1 - self.a}
        self.di, self.dj = (x, y), (y, x)
        self.dc = {"dpc": 1 - self.c}

    def barrier(self):
        sem = pltpu.get_barrier_semaphore()
        for dev in (self.di[0], self.di[1], self.dc):
            pl.semaphore_signal(sem, inc=1, device_id=dev, device_id_type=MESH)
        pl.semaphore_wait(sem, 3)

    def rows_i(self, h, i):
        return pl.ds(pl.multiple_of(h * HR + i * IR, JR), IR)

    def rows_j(self, h, i, j):
        return pl.ds(pl.multiple_of(h * HR + i * IR + j * JR, JR), JR)

    def p0(self, slot, aslot):
        return pltpu.make_async_remote_copy(self.acc.at[aslot, 1 - self.c], self.rx0.at[slot], self.sem0.at[slot, 0], self.sem0.at[slot, 1], device_id=self.dc, device_id_type=MESH)

    def px(self, phase, h, slot, aslot=None):
        i, j = self.mi[h], self.mj[h]
        if phase == 1:
            src, dst, dev = self.acc.at[aslot, self.c, self.rows_i(h, 1 - i)], self.rx1.at[slot, h], self.di[h]
        elif phase == 2:
            src, dst, dev = self.acc.at[aslot, self.c, self.rows_j(h, i, 1 - j)], self.rx2.at[slot, h], self.dj[h]
        elif phase == 3:
            src = dst = self.res.at[slot, self.rows_j(h, i, j)]
            dev = self.dj[h]
        else:
            src = dst = self.res.at[slot, self.rows_i(h, i)]
            dev = self.di[h]
        return pltpu.make_async_remote_copy(src, dst, self.semx.at[phase - 1, slot, h, 0], self.semx.at[phase - 1, slot, h, 1], device_id=dev, device_id_type=MESH)

    def p5(self, slot, idx):
        src, dst = self.res.at[slot], self.red.at[idx, self.c]
        return (
            pltpu.make_async_remote_copy(src, dst, self.sem5.at[slot, 0], self.sem5.at[slot, 1], device_id=self.dc, device_id_type=MESH),
            pltpu.make_async_copy(src, dst, self.sem5.at[slot, 2]),
        )

    def start0(self, slot, aslot):
        self.p0(slot, aslot).start()

    def start1(self, slot, aslot):
        self.p0(slot, aslot).wait()
        for h in range(2):
            sl = self.rows_i(h, 1 - self.mi[h])
            self.acc[aslot, self.c, sl, :] += self.rx0[slot, sl, :]
        for h in range(2):
            self.px(1, h, slot, aslot).start()
        for h in range(2):
            sl = self.rows_i(h, self.mi[h])
            self.acc[aslot, self.c, sl, :] += self.rx0[slot, sl, :]

    def start2(self, slot, aslot):
        for h in range(2):
            self.px(1, h, slot, aslot).wait()
        for h in range(2):
            sl = self.rows_i(h, self.mi[h])
            self.acc[aslot, self.c, sl, :] += self.rx1[slot, h]
        for h in range(2):
            self.px(2, h, slot, aslot).start()

    def end2(self, slot, aslot):
        for h in range(2):
            self.px(2, h, slot, aslot).wait()
        for h in range(2):
            sl = self.rows_j(h, self.mi[h], self.mj[h])
            self.res[slot, sl, :] = (self.acc[aslot, self.c, sl, :] + self.rx2[slot, h]) * 0.125

    def start3(self, slot):
        for h in range(2):
            self.px(3, h, slot).start()

    def start4(self, slot):
        for h in range(2):
            self.px(3, h, slot).wait()
        for h in range(2):
            self.px(4, h, slot).start()

    def start5(self, slot, idx):
        for h in range(2):
            self.px(4, h, slot).wait()
        for cp in self.p5(slot, idx):
            cp.start()

    def wait5(self, slot, idx):
        for cp in self.p5(slot, idx):
            cp.wait()


def comm_steps(cm, c, t, ev, *, acc_in, res_in, slots, end=False):
    cur, fin = lax.rem(c + 1, 2), lax.rem(c, 2)
    aslot = cur if slots == 2 else 0
    if acc_in:
        has_cur = has_fin = None
        idx = 0
    else:
        has_cur = c >= 1
        has_fin = (c >= 2) | (c == 0) if res_in else c >= 2
        idx = jnp.where(c == 0, 0, c - 1) if res_in else jnp.maximum(c - 2, 0)
    events = [
        ("s0", has_cur, lambda: cm.start0(cur, aslot)),
        ("s3", has_fin, lambda: cm.start3(fin)),
        ("s1", has_cur, lambda: cm.start1(cur, aslot)),
        ("s4", has_fin, lambda: cm.start4(fin)),
        ("s2", has_cur, lambda: cm.start2(cur, aslot)),
        ("s5", has_fin, lambda: cm.start5(fin, idx)),
        ("w5", has_fin, lambda: cm.wait5(fin, idx)),
        ("e2", has_cur, lambda: cm.end2(cur, aslot)),
    ]
    for key, cond, f in sorted(events, key=lambda e: ev[e[0]]):
        if (ev[key] >= SLOTS) != end:
            continue
        pred = t == (SLOTS - 1 if end else ev[key])
        pl.when(pred if cond is None else pred & cond)(f)


def load(cm, acc_in, res_in):
    cps = []
    if acc_in is not None:
        cps.append(pltpu.make_async_copy(acc_in, cm.acc.at[0], cm.seml.at[0]))
    if res_in is not None:
        cps.append(pltpu.make_async_copy(res_in, cm.res.at[0], cm.seml.at[1]))
    for cp in cps:
        cp.start()
    for cp in cps:
        cp.wait()


def store(cm, acc_out, aslot, res_out, rslot):
    cps = []
    if acc_out is not None:
        cps.append(pltpu.make_async_copy(cm.acc.at[aslot], acc_out, cm.seml.at[0]))
    if res_out is not None:
        cps.append(pltpu.make_async_copy(cm.res.at[rslot], res_out, cm.seml.at[1]))
    for cp in cps:
        cp.start()
    for cp in cps:
        cp.wait()


SLOTS = 8
SR = N // SLOTS
EV = {"s0": 0, "s3": 0, "s1": 1, "s4": 2, "s2": 5, "s5": 6, "w5": 7, "e2": 8}
EV4 = {"s0": 0, "s3": 0, "s1": 1, "s4": 2, "s2": 6, "s5": 7, "w5": 8, "e2": 8}
EV5 = {"s0": 0, "s3": 0, "s1": 1, "s4": 2, "s2": 5, "s5": 6, "w5": 7, "e2": 7}


def slots_of(rows, body):
    n = rows // SR

    def one(i, carry):
        body(i, pl.multiple_of(i * SR, SR))
        return carry

    if n == 1:
        body(0, 0)
    else:
        lax.fori_loop(0, n, one, 0)


def accumulate(n, dd, ee, pp):
    for j in range(n):
        dd(j)
        if j > 0:
            ee(j - 1)
        if j > 1:
            pp(j - 2)
    ee(n - 1)
    if n > 1:
        pp(n - 2)
    pp(n - 1)


def k2(h2_ref, g_ref, w3_ref, w4_ref, da3_ref, red, acc_out, res_out, a_scr, d_scr, h_scr, *scr, sub, ev):
    c, s = pl.program_id(0), pl.program_id(1)
    cm = Comm(scr, red)
    acc = cm.acc
    pl.when((c == 0) & (s == 0))(cm.barrier)
    slot = lax.rem(c, 2)
    n = h2_ref.shape[0] // SR

    def body(i, r0):
        t = s * n + i
        comm_steps(cm, c, t, ev, acc_in=False, res_in=False, slots=2)

        @pl.when(t == 0)
        def _():
            acc[slot] = jnp.zeros(acc.shape[1:], f32)

        def dd(j):
            sl, ss = pl.ds(r0 + j * sub, sub), pl.ds(j * sub, sub)
            a_scr[ss, :] = nn(h2_ref[sl, :], w3_ref[...]).astype(bf)
            d_scr[ss, :] = nt(g_ref[sl, :], w4_ref[...]).astype(bf)

        def ee(j):
            sl, ss = pl.ds(r0 + j * sub, sub), pl.ds(j * sub, sub)
            h, da = gelu_both(a_scr[ss, :].astype(f32), d_scr[ss, :].astype(f32))
            h_scr[ss, :] = h.astype(bf)
            da3_ref[sl, :] = da.astype(bf)

        def pp(j):
            sl, ss = pl.ds(r0 + j * sub, sub), pl.ds(j * sub, sub)
            acc[slot, 1] += tn(h_scr[ss, :], g_ref[sl, :])
            acc[slot, 0] += tn(h2_ref[sl, :], da3_ref[sl, :])

        accumulate(SR // sub, dd, ee, pp)
        comm_steps(cm, c, t, ev, acc_in=False, res_in=False, slots=2, end=True)

    slots_of(h2_ref.shape[0], body)

    @pl.when((c == NC - 1) & (s == pl.num_programs(1) - 1))
    def _():
        store(cm, acc_out, (NC - 1) % 2, res_out, NC % 2)


def any_spec():
    return pl.BlockSpec(memory_space=pltpu.HBM)


def red_shape(n):
    return jax.ShapeDtypeStruct((n, 2, FC, D), f32)


ACC_SHAPE = jax.ShapeDtypeStruct((2, FC, D), f32)
RES_SHAPE = jax.ShapeDtypeStruct((FC, D), f32)


def params(cid):
    return pltpu.CompilerParams(vmem_limit_bytes=VMEM_BYTES, collective_id=cid, has_side_effects=True)


def call_k2(h2, g, w3, w4, R=1024, sub=256):
    row = pl.BlockSpec((R, D), lambda c, r: (r, 0))
    return pl.pallas_call(
        functools.partial(k2, sub=sub, ev=EV),
        grid=(NC, N // R),
        in_specs=[row, row, pl.BlockSpec((D, FC), lambda c, r: (0, c)), pl.BlockSpec((FC, D), lambda c, r: (c, 0))],
        out_specs=[pl.BlockSpec((R, FC), lambda c, r: (r, c)), any_spec(), any_spec(), any_spec()],
        out_shape=[jax.ShapeDtypeStruct((N, F), bf), red_shape(2), ACC_SHAPE, RES_SHAPE],
        scratch_shapes=[pltpu.VMEM((SR, FC), bf)] * 3 + comm_scratch(2),
        compiler_params=params(0),
        cost_estimate=pl.CostEstimate(flops=8 * N * D * F, bytes_accessed=2 * N * (F + 8 * D), transcendentals=N * F),
        name="k2",
    )(h2, g, w3, w4)


def k3(a_ref, w_ref, r_ref, acc_in, res_in, o_ref, red, *rest, sub, ev, last):
    res_out, scr = (None, rest) if last else (rest[0], rest[1:])
    s = pl.program_id(0)
    cm = Comm(scr, red)

    @pl.when(s == 0)
    def _():
        load(cm, acc_in, res_in)
        cm.barrier()

    n = a_ref.shape[0] // SR

    def body(i, r0):
        t = s * n + i
        comm_steps(cm, 0, t, ev, acc_in=True, res_in=True, slots=1)
        if last:
            pl.when(t == ev["e2"])(lambda: cm.start3(1))
        for j in range(SR // sub):
            sl = pl.ds(r0 + j * sub, sub)
            o_ref[sl, :] = (nt(a_ref[sl, :], w_ref[...]) + r_ref[sl, :].astype(f32)).astype(bf)
        comm_steps(cm, 0, t, ev, acc_in=True, res_in=True, slots=1, end=True)

    slots_of(a_ref.shape[0], body)

    @pl.when(s == pl.num_programs(0) - 1)
    def _():
        if last:
            cm.start4(1)
            cm.start5(1, 1)
            cm.wait5(1, 1)
        else:
            store(cm, None, None, res_out, 1)


def call_k3(a, w, res, acc_in, res_in, last, cid, R=1024, sub=512):
    row = pl.BlockSpec((R, D), lambda r: (r, 0))
    return pl.pallas_call(
        functools.partial(k3, sub=sub, ev=EV5 if last else EV, last=last),
        grid=(N // R,),
        in_specs=[pl.BlockSpec((R, F), lambda r: (r, 0)), pl.BlockSpec((D, F), lambda r: (0, 0)), row, any_spec(), any_spec()],
        out_specs=[row, any_spec()] + ([] if last else [any_spec()]),
        out_shape=[jax.ShapeDtypeStruct((N, D), bf), red_shape(2 if last else 1)] + ([] if last else [RES_SHAPE]),
        scratch_shapes=comm_scratch(1),
        compiler_params=params(cid),
        cost_estimate=pl.CostEstimate(flops=2 * N * D * F, bytes_accessed=2 * N * (F + 2 * D), transcendentals=0),
        name="k5" if last else "k3",
    )(a, w, res, acc_in, res_in)


def k4(x_ref, dh2_ref, a1_ref, w2_ref, res_in, da1_ref, red, acc_out, res_out, d_scr, h_scr, *scr, sub, ev):
    c, s = pl.program_id(0), pl.program_id(1)
    cm = Comm(scr, red)
    acc = cm.acc

    @pl.when((c == 0) & (s == 0))
    def _():
        load(cm, None, res_in)
        cm.barrier()

    slot = lax.rem(c, 2)
    n = x_ref.shape[0] // SR

    def body(i, r0):
        t = s * n + i
        comm_steps(cm, c, t, ev, acc_in=False, res_in=True, slots=2)

        @pl.when(t == 0)
        def _():
            acc[slot] = jnp.zeros(acc.shape[1:], f32)

        def dd(j):
            sl, ss = pl.ds(r0 + j * sub, sub), pl.ds(j * sub, sub)
            d_scr[ss, :] = nt(dh2_ref[sl, :], w2_ref[...]).astype(bf)

        def ee(j):
            sl, ss = pl.ds(r0 + j * sub, sub), pl.ds(j * sub, sub)
            h, da = gelu_both(a1_ref[sl, :].astype(f32), d_scr[ss, :].astype(f32))
            h_scr[ss, :] = h.astype(bf)
            da1_ref[sl, :] = da.astype(bf)

        def pp(j):
            sl, ss = pl.ds(r0 + j * sub, sub), pl.ds(j * sub, sub)
            acc[slot, 1] += tn(h_scr[ss, :], dh2_ref[sl, :])
            acc[slot, 0] += tn(x_ref[sl, :], da1_ref[sl, :])

        accumulate(SR // sub, dd, ee, pp)
        comm_steps(cm, c, t, ev, acc_in=False, res_in=True, slots=2, end=True)

    slots_of(x_ref.shape[0], body)

    @pl.when((c == NC - 1) & (s == pl.num_programs(1) - 1))
    def _():
        store(cm, acc_out, (NC - 1) % 2, res_out, NC % 2)


def call_k4(x, dh2, a1, w2, res_in, R=1024, sub=512):
    row = pl.BlockSpec((R, D), lambda c, r: (r, 0))
    blk = pl.BlockSpec((R, FC), lambda c, r: (r, c))
    return pl.pallas_call(
        functools.partial(k4, sub=sub, ev=EV4),
        grid=(NC, N // R),
        in_specs=[row, row, blk, pl.BlockSpec((FC, D), lambda c, r: (c, 0)), any_spec()],
        out_specs=[blk, any_spec(), any_spec(), any_spec()],
        out_shape=[jax.ShapeDtypeStruct((N, F), bf), red_shape(3), ACC_SHAPE, RES_SHAPE],
        scratch_shapes=[pltpu.VMEM((SR, FC), bf)] * 2 + comm_scratch(2),
        compiler_params=params(2),
        cost_estimate=pl.CostEstimate(flops=6 * N * D * F, bytes_accessed=2 * N * (2 * F + 8 * D), transcendentals=N * F),
        name="k4",
    )(x, dh2, a1, w2, res_in)


PQ = 2


def place(r2, r3, r4a, r4b, r5, dx_in, dw1, dw2, dw3, dw4, dx):
    c = pl.program_id(0) // PQ
    dx[...] = dx_in[...]

    def put(cond, src, wa, wb):
        @pl.when(cond)
        def _():
            wa[...] = src[0, 0]
            wb[...] = src[0, 1]

    put(c < 2, r2, dw3, dw4)
    put(c == 2, r3, dw3, dw4)
    put(c == 3, r4a, dw3, dw4)
    put(c < 2, r4b, dw1, dw2)
    put(c >= 2, r5, dw1, dw2)


def call_place(r2, r3, r4, r5, dx):
    rows = FC // PQ

    def spec(lo, n, first):
        def index(t):
            k = jnp.clip(t, PQ * lo, PQ * (lo + n) - 1)
            return first + k // PQ - lo, 0, lax.rem(k, PQ), 0

        return pl.BlockSpec((1, 2, rows, D), index)

    row = pl.BlockSpec((N // (NC * PQ), D), lambda t: (t, 0))
    wide = pl.BlockSpec((rows, FC), lambda t: (lax.rem(t, PQ), t // PQ))
    tall = pl.BlockSpec((rows, D), lambda t: (t, 0))
    return pl.pallas_call(
        place,
        grid=(NC * PQ,),
        in_specs=[spec(0, 2, 0), spec(2, 1, 0), spec(3, 1, 0), spec(0, 2, 1), spec(2, 2, 0), row],
        out_specs=[wide, tall, wide, tall, row],
        out_shape=[jax.ShapeDtypeStruct((D, F), f32), jax.ShapeDtypeStruct((F, D), f32)] * 2 + [jax.ShapeDtypeStruct((N, D), bf)],
        compiler_params=pltpu.CompilerParams(vmem_limit_bytes=VMEM_BYTES),
        name="place",
    )(r2, r3, r4, r4, r5, dx)


def solution(mesh):
    rows = P(("mp", "dpa", "dpb", "dpc"), None)
    wspec = P("mp", None)

    def local(x, g, w1, w2, w3, w4):
        a1, h2 = call_k1(x, w1, w2)
        da3, r2, acc, res = call_k2(h2, g, w3, w4)
        dh2, r3, res = call_k3(da3, w3, g, acc, res, False, 1)
        da1, r4, acc, res = call_k4(x, dh2, a1, w2, res)
        dx, r5 = call_k3(da1, w1, dh2, acc, res, True, 3)
        return tuple(call_place(r2, r3, r4, r5, dx))

    return jax.shard_map(local, mesh=mesh, in_specs=(rows, rows, wspec, wspec, wspec, wspec), out_specs=(wspec, wspec, wspec, wspec, rows), check_vma=False)
```

```python
import functools

import jax
import jax.numpy as jnp
from jax import lax
from jax.experimental import pallas as pl
from jax.experimental.pallas import tpu as pltpu
from jax.sharding import PartitionSpec as P

f32 = jnp.float32
bf = jnp.bfloat16
D = 768
F = 3072
N = 8192
FC = 768
NC = F // FC
C1 = 0.7978845608028654
C2 = C1 * 0.044715
MESH = pl.DeviceIdType.MESH
HR, IR, JR = 384, 192, 96
VMEM_BYTES = 63 * 2**20


def nn(a, b):
    return lax.dot_general(a, b, (((1,), (0,)), ((), ())), preferred_element_type=f32)


def nt(a, b):
    return lax.dot_general(a, b, (((1,), (1,)), ((), ())), preferred_element_type=f32)


def tn(a, b):
    return lax.dot_general(a, b, (((0,), (0,)), ((), ())), preferred_element_type=f32)


def gelu_f(x):
    t = jnp.tanh(x * (C1 + C2 * (x * x)))
    return (0.5 * x) * (1.0 + t)


def gelu_both(x, d):
    x2 = x * x
    t = jnp.tanh(x * (C1 + C2 * x2))
    cdf = 0.5 + 0.5 * t
    h = x * cdf
    return h, (cdf + (h * (1.0 - t)) * (C1 + (3.0 * C2) * x2)) * d


def k1(x_ref, w1_ref, w2_ref, a1_ref, h2_ref, h1_scr, *, sub, fch):
    for j in range(x_ref.shape[0] // sub):
        sl = pl.ds(j * sub, sub)
        for f in range(F // fch):
            fs = pl.ds(f * fch, fch)
            a1_ref[sl, fs] = nn(x_ref[sl, :], w1_ref[:, fs]).astype(bf)
            h1_scr[sl, fs] = gelu_f(a1_ref[sl, fs].astype(f32)).astype(bf)
        h2_ref[sl, :] = (nn(h1_scr[sl, :], w2_ref[...]) + x_ref[sl, :].astype(f32)).astype(bf)


def call_k1(x, w1, w2, R=1024, sub=512, fch=768):
    return pl.pallas_call(
        functools.partial(k1, sub=sub, fch=fch),
        grid=(N // R,),
        in_specs=[pl.BlockSpec((R, D), lambda r: (r, 0)), pl.BlockSpec((D, F), lambda r: (0, 0)), pl.BlockSpec((F, D), lambda r: (0, 0))],
        out_specs=[pl.BlockSpec((R, F), lambda r: (r, 0)), pl.BlockSpec((R, D), lambda r: (r, 0))],
        out_shape=[jax.ShapeDtypeStruct((N, F), bf), jax.ShapeDtypeStruct((N, D), bf)],
        scratch_shapes=[pltpu.VMEM((R, F), bf)],
        compiler_params=pltpu.CompilerParams(vmem_limit_bytes=VMEM_BYTES),
        cost_estimate=pl.CostEstimate(flops=4 * N * D * F, bytes_accessed=2 * N * (F + 2 * D), transcendentals=N * F),
        name="k1",
    )(x, w1, w2)


def comm_scratch(slots):
    sem = pltpu.SemaphoreType.DMA
    return [
        pltpu.VMEM((slots, 2, FC, D), f32),
        pltpu.VMEM((2, FC, D), f32),
        pltpu.VMEM((2, 2, IR, D), f32),
        pltpu.VMEM((2, 2, JR, D), f32),
        pltpu.VMEM((2, FC, D), f32),
        sem((2, 2)),
        sem((4, 2, 2, 2)),
        sem((2, 3)),
        sem((2,)),
    ]


class Comm:
    def __init__(self, scr, red):
        self.acc, self.rx0, self.rx1, self.rx2, self.res, self.sem0, self.semx, self.sem5, self.seml = scr
        self.red = red
        self.a, self.b, self.c = lax.axis_index("dpa"), lax.axis_index("dpb"), lax.axis_index("dpc")
        self.mi, self.mj = (self.b, self.a), (self.a, self.b)
        x, y = {"dpb": 1 - self.b}, {"dpa": 1 - self.a}
        self.di, self.dj = (x, y), (y, x)
        self.dc = {"dpc": 1 - self.c}

    def barrier(self):
        sem = pltpu.get_barrier_semaphore()
        for dev in (self.di[0], self.di[1], self.dc):
            pl.semaphore_signal(sem, inc=1, device_id=dev, device_id_type=MESH)
        pl.semaphore_wait(sem, 3)

    def rows_i(self, h, i):
        return pl.ds(pl.multiple_of(h * HR + i * IR, JR), IR)

    def rows_j(self, h, i, j):
        return pl.ds(pl.multiple_of(h * HR + i * IR + j * JR, JR), JR)

    def p0(self, slot, aslot):
        return pltpu.make_async_remote_copy(self.acc.at[aslot, 1 - self.c], self.rx0.at[slot], self.sem0.at[slot, 0], self.sem0.at[slot, 1], device_id=self.dc, device_id_type=MESH)

    def px(self, phase, h, slot, aslot=None):
        i, j = self.mi[h], self.mj[h]
        if phase == 1:
            src, dst, dev = self.acc.at[aslot, self.c, self.rows_i(h, 1 - i)], self.rx1.at[slot, h], self.di[h]
        elif phase == 2:
            src, dst, dev = self.acc.at[aslot, self.c, self.rows_j(h, i, 1 - j)], self.rx2.at[slot, h], self.dj[h]
        elif phase == 3:
            src = dst = self.res.at[slot, self.rows_j(h, i, j)]
            dev = self.dj[h]
        else:
            src = dst = self.res.at[slot, self.rows_i(h, i)]
            dev = self.di[h]
        return pltpu.make_async_remote_copy(src, dst, self.semx.at[phase - 1, slot, h, 0], self.semx.at[phase - 1, slot, h, 1], device_id=dev, device_id_type=MESH)

    def p5(self, slot, idx):
        src, dst = self.res.at[slot], self.red.at[idx, self.c]
        return (
            pltpu.make_async_remote_copy(src, dst, self.sem5.at[slot, 0], self.sem5.at[slot, 1], device_id=self.dc, device_id_type=MESH),
            pltpu.make_async_copy(src, dst, self.sem5.at[slot, 2]),
        )

    def start0(self, slot, aslot):
        self.p0(slot, aslot).start()

    def start1(self, slot, aslot):
        self.p0(slot, aslot).wait()
        for h in range(2):
            sl = self.rows_i(h, 1 - self.mi[h])
            self.acc[aslot, self.c, sl, :] += self.rx0[slot, sl, :]
        for h in range(2):
            self.px(1, h, slot, aslot).start()
        for h in range(2):
            sl = self.rows_i(h, self.mi[h])
            self.acc[aslot, self.c, sl, :] += self.rx0[slot, sl, :]

    def start2(self, slot, aslot):
        for h in range(2):
            self.px(1, h, slot, aslot).wait()
        for h in range(2):
            sl = self.rows_i(h, self.mi[h])
            self.acc[aslot, self.c, sl, :] += self.rx1[slot, h]
        for h in range(2):
            self.px(2, h, slot, aslot).start()

    def end2(self, slot, aslot):
        for h in range(2):
            self.px(2, h, slot, aslot).wait()
        for h in range(2):
            sl = self.rows_j(h, self.mi[h], self.mj[h])
            self.res[slot, sl, :] = (self.acc[aslot, self.c, sl, :] + self.rx2[slot, h]) * 0.125

    def start3(self, slot):
        for h in range(2):
            self.px(3, h, slot).start()

    def start4(self, slot):
        for h in range(2):
            self.px(3, h, slot).wait()
        for h in range(2):
            self.px(4, h, slot).start()

    def start5(self, slot, idx):
        for h in range(2):
            self.px(4, h, slot).wait()
        for cp in self.p5(slot, idx):
            cp.start()

    def wait5(self, slot, idx):
        for cp in self.p5(slot, idx):
            cp.wait()


def comm_steps(cm, c, t, ev, *, acc_in, res_in, slots, end=False):
    cur, fin = lax.rem(c + 1, 2), lax.rem(c, 2)
    aslot = cur if slots == 2 else 0
    if acc_in:
        has_cur = has_fin = None
        idx = 0
    else:
        has_cur = c >= 1
        has_fin = (c >= 2) | (c == 0) if res_in else c >= 2
        idx = jnp.where(c == 0, 0, c - 1) if res_in else jnp.maximum(c - 2, 0)
    events = [
        ("s0", has_cur, lambda: cm.start0(cur, aslot)),
        ("s3", has_fin, lambda: cm.start3(fin)),
        ("s1", has_cur, lambda: cm.start1(cur, aslot)),
        ("s4", has_fin, lambda: cm.start4(fin)),
        ("s2", has_cur, lambda: cm.start2(cur, aslot)),
        ("s5", has_fin, lambda: cm.start5(fin, idx)),
        ("w5", has_fin, lambda: cm.wait5(fin, idx)),
        ("e2", has_cur, lambda: cm.end2(cur, aslot)),
    ]
    for key, cond, f in sorted(events, key=lambda e: ev[e[0]]):
        if (ev[key] >= SLOTS) != end:
            continue
        pred = t == (SLOTS - 1 if end else ev[key])
        pl.when(pred if cond is None else pred & cond)(f)


def load(cm, acc_in, res_in):
    cps = []
    if acc_in is not None:
        cps.append(pltpu.make_async_copy(acc_in, cm.acc.at[0], cm.seml.at[0]))
    if res_in is not None:
        cps.append(pltpu.make_async_copy(res_in, cm.res.at[0], cm.seml.at[1]))
    for cp in cps:
        cp.start()
    for cp in cps:
        cp.wait()


def store(cm, acc_out, aslot, res_out, rslot):
    cps = []
    if acc_out is not None:
        cps.append(pltpu.make_async_copy(cm.acc.at[aslot], acc_out, cm.seml.at[0]))
    if res_out is not None:
        cps.append(pltpu.make_async_copy(cm.res.at[rslot], res_out, cm.seml.at[1]))
    for cp in cps:
        cp.start()
    for cp in cps:
        cp.wait()


SLOTS = 8
SR = N // SLOTS
EV = {"s0": 0, "s3": 0, "s1": 1, "s4": 2, "s2": 5, "s5": 6, "w5": 7, "e2": 8}
EV4 = {"s0": 0, "s3": 0, "s1": 1, "s4": 2, "s2": 6, "s5": 7, "w5": 8, "e2": 8}
EV5 = {"s0": 0, "s3": 0, "s1": 1, "s4": 2, "s2": 5, "s5": 6, "w5": 7, "e2": 7}


def slots_of(rows, body):
    n = rows // SR

    def one(i, carry):
        body(i, pl.multiple_of(i * SR, SR))
        return carry

    if n == 1:
        body(0, 0)
    else:
        lax.fori_loop(0, n, one, 0)


def accumulate(n, dd, ee, pp, group=1):
    done = 0
    for j in range(n):
        dd(j)
        if j > 0:
            ee(j - 1)
        if j - 1 >= done + group:
            pp(done // group)
            done += group
    ee(n - 1)
    while done < n:
        pp(done // group)
        done += group


def k2(h2_ref, g_ref, w3_ref, w4_ref, da3_ref, red, acc_out, res_out, a_scr, d_scr, h_scr, *scr, sub, ev):
    c, s = pl.program_id(0), pl.program_id(1)
    cm = Comm(scr, red)
    acc = cm.acc
    pl.when((c == 0) & (s == 0))(cm.barrier)
    slot = lax.rem(c, 2)
    n = h2_ref.shape[0] // SR

    def body(i, r0):
        t = s * n + i
        comm_steps(cm, c, t, ev, acc_in=False, res_in=False, slots=2)

        @pl.when(t == 0)
        def _():
            acc[slot] = jnp.zeros(acc.shape[1:], f32)

        def dd(j):
            sl, ss = pl.ds(r0 + j * sub, sub), pl.ds(j * sub, sub)
            a_scr[ss, :] = nn(h2_ref[sl, :], w3_ref[...]).astype(bf)
            d_scr[ss, :] = nt(g_ref[sl, :], w4_ref[...]).astype(bf)

        def ee(j):
            sl, ss = pl.ds(r0 + j * sub, sub), pl.ds(j * sub, sub)
            h, da = gelu_both(a_scr[ss, :].astype(f32), d_scr[ss, :].astype(f32))
            h_scr[ss, :] = h.astype(bf)
            da3_ref[sl, :] = da.astype(bf)

        def pp(j):
            sl, ss = pl.ds(r0 + j * 2 * sub, 2 * sub), pl.ds(j * 2 * sub, 2 * sub)
            acc[slot, 1] += tn(h_scr[ss, :], g_ref[sl, :])
            acc[slot, 0] += tn(h2_ref[sl, :], da3_ref[sl, :])

        accumulate(SR // sub, dd, ee, pp, 2)
        comm_steps(cm, c, t, ev, acc_in=False, res_in=False, slots=2, end=True)

    slots_of(h2_ref.shape[0], body)

    @pl.when((c == NC - 1) & (s == pl.num_programs(1) - 1))
    def _():
        store(cm, acc_out, (NC - 1) % 2, res_out, NC % 2)


def any_spec():
    return pl.BlockSpec(memory_space=pltpu.HBM)


def red_shape(n):
    return jax.ShapeDtypeStruct((n, 2, FC, D), f32)


ACC_SHAPE = jax.ShapeDtypeStruct((2, FC, D), f32)
RES_SHAPE = jax.ShapeDtypeStruct((FC, D), f32)


def params(cid):
    return pltpu.CompilerParams(vmem_limit_bytes=VMEM_BYTES, collective_id=cid, has_side_effects=True)


def call_k2(h2, g, w3, w4, R=1024, sub=256):
    row = pl.BlockSpec((R, D), lambda c, r: (r, 0))
    return pl.pallas_call(
        functools.partial(k2, sub=sub, ev=EV),
        grid=(NC, N // R),
        in_specs=[row, row, pl.BlockSpec((D, FC), lambda c, r: (0, c)), pl.BlockSpec((FC, D), lambda c, r: (c, 0))],
        out_specs=[pl.BlockSpec((R, FC), lambda c, r: (r, c)), any_spec(), any_spec(), any_spec()],
        out_shape=[jax.ShapeDtypeStruct((N, F), bf), red_shape(2), ACC_SHAPE, RES_SHAPE],
        scratch_shapes=[pltpu.VMEM((SR, FC), bf)] * 3 + comm_scratch(2),
        compiler_params=params(0),
        cost_estimate=pl.CostEstimate(flops=8 * N * D * F, bytes_accessed=2 * N * (F + 8 * D), transcendentals=N * F),
        name="k2",
    )(h2, g, w3, w4)


def k3(a_ref, w_ref, r_ref, acc_in, res_in, o_ref, red, *rest, sub, ev, last):
    res_out, scr = (None, rest) if last else (rest[0], rest[1:])
    s = pl.program_id(0)
    cm = Comm(scr, red)

    @pl.when(s == 0)
    def _():
        load(cm, acc_in, res_in)
        cm.barrier()

    n = a_ref.shape[0] // SR

    def body(i, r0):
        t = s * n + i
        comm_steps(cm, 0, t, ev, acc_in=True, res_in=True, slots=1)
        if last:
            pl.when(t == ev["e2"])(lambda: cm.start3(1))
        for j in range(SR // sub):
            sl = pl.ds(r0 + j * sub, sub)
            o_ref[sl, :] = (nt(a_ref[sl, :], w_ref[...]) + r_ref[sl, :].astype(f32)).astype(bf)
        comm_steps(cm, 0, t, ev, acc_in=True, res_in=True, slots=1, end=True)

    slots_of(a_ref.shape[0], body)

    @pl.when(s == pl.num_programs(0) - 1)
    def _():
        if last:
            cm.start4(1)
            cm.start5(1, 1)
            cm.wait5(1, 1)
        else:
            store(cm, None, None, res_out, 1)


def call_k3(a, w, res, acc_in, res_in, last, cid, R=1024, sub=512):
    row = pl.BlockSpec((R, D), lambda r: (r, 0))
    return pl.pallas_call(
        functools.partial(k3, sub=sub, ev=EV5 if last else EV, last=last),
        grid=(N // R,),
        in_specs=[pl.BlockSpec((R, F), lambda r: (r, 0)), pl.BlockSpec((D, F), lambda r: (0, 0)), row, any_spec(), any_spec()],
        out_specs=[row, any_spec()] + ([] if last else [any_spec()]),
        out_shape=[jax.ShapeDtypeStruct((N, D), bf), red_shape(2 if last else 1)] + ([] if last else [RES_SHAPE]),
        scratch_shapes=comm_scratch(1),
        compiler_params=params(cid),
        cost_estimate=pl.CostEstimate(flops=2 * N * D * F, bytes_accessed=2 * N * (F + 2 * D), transcendentals=0),
        name="k5" if last else "k3",
    )(a, w, res, acc_in, res_in)


def k4(x_ref, dh2_ref, a1_ref, w2_ref, res_in, da1_ref, red, acc_out, res_out, d_scr, h_scr, *scr, sub, ev):
    c, s = pl.program_id(0), pl.program_id(1)
    cm = Comm(scr, red)
    acc = cm.acc

    @pl.when((c == 0) & (s == 0))
    def _():
        load(cm, None, res_in)
        cm.barrier()

    slot = lax.rem(c, 2)
    n = x_ref.shape[0] // SR

    def body(i, r0):
        t = s * n + i
        comm_steps(cm, c, t, ev, acc_in=False, res_in=True, slots=2)

        @pl.when(t == 0)
        def _():
            acc[slot] = jnp.zeros(acc.shape[1:], f32)

        def dd(j):
            sl, ss = pl.ds(r0 + j * sub, sub), pl.ds(j * sub, sub)
            d_scr[ss, :] = nt(dh2_ref[sl, :], w2_ref[...]).astype(bf)

        def ee(j):
            sl, ss = pl.ds(r0 + j * sub, sub), pl.ds(j * sub, sub)
            h, da = gelu_both(a1_ref[sl, :].astype(f32), d_scr[ss, :].astype(f32))
            h_scr[ss, :] = h.astype(bf)
            da1_ref[sl, :] = da.astype(bf)

        def pp(j):
            sl, ss = pl.ds(r0 + j * sub, sub), pl.ds(j * sub, sub)
            acc[slot, 1] += tn(h_scr[ss, :], dh2_ref[sl, :])
            acc[slot, 0] += tn(x_ref[sl, :], da1_ref[sl, :])

        accumulate(SR // sub, dd, ee, pp)
        comm_steps(cm, c, t, ev, acc_in=False, res_in=True, slots=2, end=True)

    slots_of(x_ref.shape[0], body)

    @pl.when((c == NC - 1) & (s == pl.num_programs(1) - 1))
    def _():
        store(cm, acc_out, (NC - 1) % 2, res_out, NC % 2)


def call_k4(x, dh2, a1, w2, res_in, R=1024, sub=512):
    row = pl.BlockSpec((R, D), lambda c, r: (r, 0))
    blk = pl.BlockSpec((R, FC), lambda c, r: (r, c))
    return pl.pallas_call(
        functools.partial(k4, sub=sub, ev=EV4),
        grid=(NC, N // R),
        in_specs=[row, row, blk, pl.BlockSpec((FC, D), lambda c, r: (c, 0)), any_spec()],
        out_specs=[blk, any_spec(), any_spec(), any_spec()],
        out_shape=[jax.ShapeDtypeStruct((N, F), bf), red_shape(3), ACC_SHAPE, RES_SHAPE],
        scratch_shapes=[pltpu.VMEM((SR, FC), bf)] * 2 + comm_scratch(2),
        compiler_params=params(2),
        cost_estimate=pl.CostEstimate(flops=6 * N * D * F, bytes_accessed=2 * N * (2 * F + 8 * D), transcendentals=N * F),
        name="k4",
    )(x, dh2, a1, w2, res_in)


PQ = 2


def place(r2, r3, r4a, r4b, r5, dx_in, dw1, dw2, dw3, dw4, dx):
    c = pl.program_id(0) // PQ
    dx[...] = dx_in[...]

    def put(cond, src, wa, wb):
        @pl.when(cond)
        def _():
            wa[...] = src[0, 0]
            wb[...] = src[0, 1]

    put(c < 2, r2, dw3, dw4)
    put(c == 2, r3, dw3, dw4)
    put(c == 3, r4a, dw3, dw4)
    put(c < 2, r4b, dw1, dw2)
    put(c >= 2, r5, dw1, dw2)


def call_place(r2, r3, r4, r5, dx):
    rows = FC // PQ

    def spec(lo, n, first):
        def index(t):
            k = jnp.clip(t, PQ * lo, PQ * (lo + n) - 1)
            return first + k // PQ - lo, 0, lax.rem(k, PQ), 0

        return pl.BlockSpec((1, 2, rows, D), index)

    row = pl.BlockSpec((N // (NC * PQ), D), lambda t: (t, 0))
    wide = pl.BlockSpec((rows, FC), lambda t: (lax.rem(t, PQ), t // PQ))
    tall = pl.BlockSpec((rows, D), lambda t: (t, 0))
    return pl.pallas_call(
        place,
        grid=(NC * PQ,),
        in_specs=[spec(0, 2, 0), spec(2, 1, 0), spec(3, 1, 0), spec(0, 2, 1), spec(2, 2, 0), row],
        out_specs=[wide, tall, wide, tall, row],
        out_shape=[jax.ShapeDtypeStruct((D, F), f32), jax.ShapeDtypeStruct((F, D), f32)] * 2 + [jax.ShapeDtypeStruct((N, D), bf)],
        compiler_params=pltpu.CompilerParams(vmem_limit_bytes=VMEM_BYTES),
        name="place",
    )(r2, r3, r4, r4, r5, dx)


def solution(mesh):
    rows = P(("mp", "dpa", "dpb", "dpc"), None)
    wspec = P("mp", None)

    def local(x, g, w1, w2, w3, w4):
        a1, h2 = call_k1(x, w1, w2)
        da3, r2, acc, res = call_k2(h2, g, w3, w4)
        dh2, r3, res = call_k3(da3, w3, g, acc, res, False, 1)
        da1, r4, acc, res = call_k4(x, dh2, a1, w2, res)
        dx, r5 = call_k3(da1, w1, dh2, acc, res, True, 3)
        return tuple(call_place(r2, r3, r4, r5, dx))

    return jax.shard_map(local, mesh=mesh, in_specs=(rows, rows, wspec, wspec, wspec, wspec), out_specs=(wspec, wspec, wspec, wspec, rows), check_vma=False)
```
